128 devices in a mesh: row: 16 (over z_hi, y, core), col: 8 (over x, z_lo).
Axes of the slice: x: 4, y: 4, z: 4 (z_hi: 2, z_lo: 2; z = z_hi * 2 + z_lo), core: 2. Of those that a mesh axis runs over, the one named last changes fastest.
Arguments:
- rotation: bfloat16 [8192, 8192], P('row', 'col'), may hold values from -0.0625 to 0.0625
- gradient: bfloat16 [8192, 8192], P('row', 'col'), may hold values from -0.0625 to 0.0625
Outputs:
- updated: float32 [8192, 2048], P('row', 'col')
- column_norms: float32 [2048], P('col')
The draws below stay inside these ranges and needn't reach their ends.
All inputs are finite; a program needn't handle non-finite values.
Results may differ from the reference program's by a relative error of at most 0.01.
Values may be sent and summed in bfloat16 or wider, within the bound.
A program may use at most 128 MiB of HBM per device.

```python
import jax
import jax.numpy as jnp
from jax import lax

N = 8192
SLAB = 2048
N_ROW = 16


def levels(key, dims, split, least, high):
    level = 1.0
    for axis_at, blocks in split:
        steps = jax.random.uniform(jax.random.fold_in(jax.random.fold_in(key, 6), axis_at), (blocks,), jnp.float32, least / len(split), high / len(split))
        level = level * jnp.repeat(jnp.exp(steps), dims[axis_at] // blocks).reshape((-1,) + (1,) * (len(dims) - 1 - axis_at))
    return level


def normal_values(own_key, extent, width, most, cuts=(), kind=jnp.bfloat16):
    values = width * jax.random.normal(own_key, extent, jnp.float32)
    if cuts:
        values = values * levels(own_key, extent, cuts, -0.22, 0.18)
    return jnp.clip(values, -most, most).astype(kind)


def setup_inputs(seed: int = 0) -> dict:
    seeds = jax.random.split(jax.random.key(seed), 3)
    return {
        "rotation": normal_values(seeds[0], (N, N), N ** -0.5, 0.0625, ((0, 16), (1, 8))),
        "gradient": normal_values(seeds[1], (N, N), N ** -0.5, 0.0625, ((0, 16), (1, 8))),
    }


def apply_generator(rotation, gradient, panel):
    block = N // N_ROW
    rot_blocks = rotation.reshape(N_ROW, block, N)
    grad_blocks = gradient.reshape(N_ROW, block, N)
    pan_blocks = panel.reshape(N_ROW, block, panel.shape[1])

    def add_block(carry, pieces):
        rot_piece, grad_piece, pan_piece = pieces
        left = jnp.dot(rot_piece.T, pan_piece, preferred_element_type=jnp.float32)
        right = jnp.dot(grad_piece.T, pan_piece, preferred_element_type=jnp.float32)
        left = lax.optimization_barrier(left.astype(jnp.bfloat16)).astype(jnp.float32)
        right = lax.optimization_barrier(right.astype(jnp.bfloat16)).astype(jnp.float32)
        return ((carry[0] + left, carry[1] + right), None)
    zeros = jnp.zeros((N, panel.shape[1]), jnp.float32)
    (left_sum, right_sum), _ = lax.scan(add_block, (zeros, zeros), (rot_blocks, grad_blocks, pan_blocks))
    left_sum = left_sum.astype(jnp.bfloat16)
    right_sum = right_sum.astype(jnp.bfloat16)
    return jnp.dot(gradient, left_sum, preferred_element_type=jnp.float32) - jnp.dot(rotation, right_sum, preferred_element_type=jnp.float32)

def reference(rotation, gradient):
    base = rotation[:, ::N // SLAB]
    base_wide = base.astype(jnp.float32)
    first = base_wide + 0.25 * apply_generator(rotation, gradient, base)
    middle = (base_wide + first).astype(jnp.bfloat16)
    updated = base_wide + 0.125 * apply_generator(rotation, gradient, middle)
    column_norms = jnp.sqrt(lax.optimization_barrier(jnp.sum(updated * updated, axis=0)))
    return (updated, column_norms)
```

```python
import jax
import jax.numpy as jnp
from jax import lax
from jax.experimental import pallas as pl
from jax.experimental.pallas import tpu as pltpu
from jax.sharding import PartitionSpec as P

MESH = pl.DeviceIdType.MESH
F32 = jnp.float32
BF16 = jnp.bfloat16
NS = 4
CH = 32
BLK = 1024
HALF = 512
TILE = 512
ITEMS = 2 * NS


def step_kernel(
    rot_hbm, grad_hbm, out_ref, norm_ref,
    rot, grad, base, panel, part, full, mine, ring_a, ring_b, swapped,
    term, term_in, kept, tail, tail_in, upd, turned, turned_in, sq, sq_y, sq_sum, sq_in,
    load_sem, pair_s, pair_r, v0_s, v0_r, v1_s, v1_r, a_s, a_r, b_s, b_r, z_s, z_r,
    c_s, c_r, e_s, e_r, t_s, t_r, w_s, w_r, u_s, u_r, n_s, n_r, m_s, m_r,
):
    row = lax.axis_index("row")
    col = lax.axis_index("col")
    core, y, zh = row % 2, (row // 2) % 4, row // 8
    x, zl = col // 2, col % 2
    up, across, down = (y + 1) % 4, (y + 2) % 4, (y + 3) % 4

    def at_row(zh_, y_, core_):
        return {"row": zh_ * 8 + y_ * 2 + core_, "col": col}

    def at_col(x_, zl_):
        return {"row": row, "col": x_ * 2 + zl_}

    pair = at_row(zh, y, 1 - core)
    y_dev = (at_row(zh, up, core), at_row(zh, down, core))
    y_q = (up, down)
    y_all = tuple(at_row(zh, (y + k) % 4, core) for k in (1, 2, 3))
    z_dev = at_row(1 - zh, y, core)
    zc_dev = at_row(1 - zh, y, 1 - core)
    x_all = tuple(at_col((x + k) % 4, zl) for k in (1, 2, 3))
    zl_dev = at_col(x, 1 - zl)

    def send(src, dst, s, r, dev):
        return pltpu.make_async_remote_copy(
            src_ref=src, dst_ref=dst, send_sem=s, recv_sem=r, device_id=dev, device_id_type=MESH
        )

    own_rows = pl.ds(pl.multiple_of(core * HALF, HALF), HALF)
    other_rows = pl.ds(pl.multiple_of((1 - core) * HALF, HALF), HALF)
    loads = [
        pltpu.make_async_copy(rot_hbm, rot.at[own_rows], load_sem.at[0]),
        pltpu.make_async_copy(grad_hbm, grad.at[own_rows], load_sem.at[1]),
    ]
    for c in loads:
        c.start()

    barrier = pltpu.get_barrier_semaphore()
    peers = (pair, *y_all, z_dev, zc_dev, *x_all, zl_dev)
    for dev in peers:
        pl.semaphore_signal(barrier, inc=1, device_id=dev, device_id_type=MESH)
    pl.semaphore_wait(barrier, len(peers))

    pairs = [
        send(m.at[own_rows], m.at[own_rows], pair_s.at[k], pair_r.at[k], pair)
        for k, m in enumerate((rot, grad))
    ]
    for c, p in zip(loads, pairs):
        c.wait()
        p.start()
    pairs[0].wait_recv()

    pick = lax.broadcasted_iota(jnp.int32, (128, HALF), 1) == 4 * lax.broadcasted_iota(
        jnp.int32, (128, HALF), 0
    )
    base[...] = (
        lax.dot_general(
            pick.astype(F32).astype(BF16),
            rot[:, pl.ds(pl.multiple_of(core * HALF, HALF), HALF)],
            (((1,), (1,)), ((), ())),
            preferred_element_type=F32,
        )
        .astype(BF16)
        .reshape(NS, CH, BLK)
    )

    def v0(i):
        k = i % NS
        return send(panel.at[k, x, zl], panel.at[k, x, zl], v0_s.at[k], v0_r.at[k], zl_dev)

    def v1(i, d):
        k = i % NS
        return send(panel.at[k, x], panel.at[k, x], v1_s.at[k, d], v1_r.at[k, d], x_all[d])

    def ra(i, h, d):
        k = i % NS
        return send(
            part.at[k, h, across, d], ring_a.at[k, h, d], a_s.at[k, h, d], a_r.at[k, h, d], y_dev[d]
        )

    def rb(i, h, d):
        k = i % NS
        return send(
            part.at[k, h, y_q[d]], ring_b.at[k, h, d], b_s.at[k, h, d], b_r.at[k, h, d], y_dev[d]
        )

    def zx(i, h):
        k = i % NS
        return send(mine.at[k, h], swapped.at[k, h], z_s.at[k, h], z_r.at[k, h], z_dev)

    def ga(i, h, d):
        k = i % NS
        return send(
            full.at[k, h, y], full.at[k, h, y], c_s.at[k, h, d], c_r.at[k, h, d], y_dev[d]
        )

    def gb(i, h, d):
        k = i % NS
        q = y_q[1 - d]
        return send(
            full.at[k, h, q, d], full.at[k, h, q, d], e_s.at[k, h, d], e_r.at[k, h, d], y_dev[d]
        )

    def tx(i, d):
        k = i % NS
        return send(
            term.at[k, (x + d + 1) % 4], term_in.at[k, d], t_s.at[k, d], t_r.at[k, d], x_all[d]
        )

    def wz(i):
        k = i % NS
        return send(tail.at[k], tail_in.at[k], w_s.at[k], w_r.at[k], zl_dev)

    for j in range(NS):
        panel[j, x, zl] = base[j]
    for j in range(NS):
        v0(j).start()
    for j in range(NS):
        v0(j).wait_recv()
        for d in range(3):
            v1(j, d).start()
    pairs[1].wait_recv()

    def project(i, h):
        k = i % NS
        held = (rot, grad)[h]
        lhs = panel[k].reshape(8 * CH, BLK)

        @pl.loop(0, BLK // TILE)
        def _(n):
            cols = pl.ds(pl.multiple_of(n * TILE, TILE), TILE)
            z = jnp.dot(lhs, held[:, cols], preferred_element_type=F32)
            part[k, h, :, :, :, cols] = z.astype(BF16).reshape(4, 2, CH, TILE)

    def apply(i):
        k = i % NS

        @pl.loop(0, BLK // TILE)
        def _(n):
            rows = pl.ds(pl.multiple_of(n * TILE, TILE), TILE)
            nt = (((1,), (1,)), ((), ()))
            t = lax.dot_general(
                full[k, 0].reshape(8 * CH, BLK), grad[rows, :], nt, preferred_element_type=F32
            ) - lax.dot_general(
                full[k, 1].reshape(8 * CH, BLK), rot[rows, :], nt, preferred_element_type=F32
            )
            term[k, :, :, :, rows] = t.astype(BF16).reshape(4, 2, CH, TILE)

    def run(i, _):
        with_b = (i >= 1) & (i <= ITEMS)
        with_c = (i >= 2) & (i <= ITEMS + 1)
        with_d = (i >= 3) & (i <= ITEMS + 2)
        with_v = (i >= NS) & (i < ITEMS)

        @pl.when(with_b)
        def _():
            it = i - 1
            for d in range(3):
                v1(it, d).wait_recv()
            for h in range(2):
                project(it, h)
                for d in range(2):
                    ra(it, h, d).start()
            v0(it).wait_send()

        @pl.when(with_d)
        def _():
            it = i - 3
            for h in range(2):
                for d in range(2):
                    ga(it, h, d).wait_recv()
                for d in range(2):
                    gb(it, h, d).start()
            for h in range(2):
                zx(it, h).wait_send()

        @pl.when(i >= NS)
        def _():
            it = i - NS
            k = it % NS
            wz(it).wait_recv()
            applied = kept[k] + tail_in[k].astype(F32)
            b = base[k].astype(F32)

            @pl.when(i < ITEMS)
            def _():
                first = b + 0.25 * applied
                panel[k, x, zl] = (b + first).astype(BF16)
                v0(i).start()

            @pl.when(i >= ITEMS)
            def _():
                upd[k] = b + 0.125 * applied

            for d in range(3):
                tx(it, d).wait_send()
            wz(it).wait_send()

        @pl.when(with_b)
        def _():
            it = i - 1
            k = it % NS
            for h in range(2):
                for d in range(2):
                    ra(it, h, d).wait_recv()
                    total = part[k, h, y_q[d], d].astype(F32) + ring_a[k, h, d].astype(F32)
                    part[k, h, y_q[d], d] = total.astype(BF16)
                    rb(it, h, d).start()
            for d in range(3):
                v1(it, d).wait_send()

        @pl.when(with_v)
        def _():
            v0(i).wait_recv()
            for d in range(3):
                v1(i, d).start()

        @pl.when(with_d)
        def _():
            it = i - 3
            for h in range(2):
                for d in range(2):
                    gb(it, h, d).wait_recv()
            apply(it)
            for d in range(3):
                tx(it, d).start()
            for h in range(2):
                for d in range(2):
                    ga(it, h, d).wait_send()

        @pl.when(with_c)
        def _():
            it = i - 2
            k = it % NS
            for h in range(2):
                zx(it, h).wait_recv()
                z = mine[k, h].astype(F32) + swapped[k, h].astype(F32)
                full[k, h, y] = z.astype(BF16)
                for d in range(2):
                    ga(it, h, d).start()
            for h in range(2):
                for d in range(2):
                    rb(it, h, d).wait_send()

        @pl.when(with_b)
        def _():
            it = i - 1
            k = it % NS
            for h in range(2):
                for d in range(2):
                    rb(it, h, d).wait_recv()
                s = part[k, h, y].astype(F32) + (
                    ring_b[k, h, 0].astype(F32) + ring_b[k, h, 1].astype(F32)
                )
                mine[k, h] = s.astype(BF16)
                zx(it, h).start()
            for h in range(2):
                for d in range(2):
                    ra(it, h, d).wait_send()

        @pl.when(with_d)
        def _():
            it = i - 3
            k = it % NS
            for d in range(3):
                tx(it, d).wait_recv()

            def summed(z):
                return (term[k, x, z].astype(F32) + term_in[k, 0, z].astype(F32)) + (
                    term_in[k, 1, z].astype(F32) + term_in[k, 2, z].astype(F32)
                )

            tail[k] = summed(1 - zl).astype(BF16)
            wz(it).start()
            kept[k] = summed(zl)
            for h in range(2):
                for d in range(2):
                    gb(it, h, d).wait_send()

        return 0

    lax.fori_loop(1, ITEMS + NS, run, 0)

    total = jnp.zeros((1, 128), F32)
    for r in range(BLK // 128):
        block = upd[:, :, r * 128 : (r + 1) * 128].reshape(128, 128).T
        turned[r * 128 : (r + 1) * 128, :] = block
        total = total + jnp.sum(block * block, axis=0, keepdims=True)
    sq[...] = jnp.broadcast_to(total, (8, 128))
    swap = send(turned.at[other_rows], turned_in, u_s.at[0], u_r.at[0], pair)
    swap.start()
    ys = [send(sq, sq_y.at[k], n_s.at[k], n_r.at[k], y_all[k]) for k in range(3)]
    for c in ys:
        c.start()
    out_ref[:, pl.ds(pl.multiple_of(core * 128, 128), 128)] = turned[own_rows, :]
    for c in ys:
        c.wait_recv()
    sq_sum[...] = (sq[...] + sq_y[0]) + (sq_y[1] + sq_y[2])
    ms = [
        send(sq_sum, sq_in.at[k], m_s.at[k], m_r.at[k], dev)
        for k, dev in enumerate((z_dev, pair, zc_dev))
    ]
    for c in ms:
        c.start()
    swap.wait_recv()
    out_ref[:, pl.ds(pl.multiple_of((1 - core) * 128, 128), 128)] = turned_in[...]
    for c in ms:
        c.wait_recv()
    own_norm = jnp.sqrt(sq_sum[0:1, :] + sq_in[0, 0:1, :])
    other_norm = jnp.sqrt(sq_in[1, 0:1, :] + sq_in[2, 0:1, :])
    norm_ref[0:1, :] = jnp.where(core == 0, own_norm, other_norm)
    norm_ref[1:2, :] = jnp.where(core == 0, other_norm, own_norm)
    for c in (*pairs, swap, *ys, *ms):
        c.wait_send()


def on_device(rotation, gradient):
    dma = pltpu.SemaphoreType.DMA

    def both(shape):
        return [dma(shape), dma(shape)]

    quarters = (4, 2, CH, BLK)
    updated, norms = pl.pallas_call(
        step_kernel,
        name="cayley_step",
        out_shape=(
            jax.ShapeDtypeStruct((HALF, 256), F32),
            jax.ShapeDtypeStruct((2, 128), F32),
        ),
        in_specs=[pl.BlockSpec(memory_space=pl.ANY)] * 2,
        out_specs=(
            pl.BlockSpec(memory_space=pltpu.VMEM),
            pl.BlockSpec(memory_space=pltpu.VMEM),
        ),
        scratch_shapes=[
            pltpu.VMEM((BLK, BLK), BF16),
            pltpu.VMEM((BLK, BLK), BF16),
            pltpu.VMEM((NS, CH, BLK), BF16),
            pltpu.VMEM((NS, *quarters), BF16),
            pltpu.VMEM((NS, 2, *quarters), BF16),
            pltpu.VMEM((NS, 2, *quarters), BF16),
            pltpu.VMEM((NS, 2, 2, CH, BLK), BF16),
            pltpu.VMEM((NS, 2, 2, CH, BLK), BF16),
            pltpu.VMEM((NS, 2, 2, 2, CH, BLK), BF16),
            pltpu.VMEM((NS, 2, 2, CH, BLK), BF16),
            pltpu.VMEM((NS, *quarters), BF16),
            pltpu.VMEM((NS, 3, 2, CH, BLK), BF16),
            pltpu.VMEM((NS, CH, BLK), F32),
            pltpu.VMEM((NS, CH, BLK), BF16),
            pltpu.VMEM((NS, CH, BLK), BF16),
            pltpu.VMEM((NS, CH, BLK), F32),
            pltpu.VMEM((BLK, 128), F32),
            pltpu.VMEM((HALF, 128), F32),
            pltpu.VMEM((8, 128), F32),
            pltpu.VMEM((3, 8, 128), F32),
            pltpu.VMEM((8, 128), F32),
            pltpu.VMEM((3, 8, 128), F32),
            dma((2,)),
            *both((2,)),
            *both((NS,)),
            *both((NS, 3)),
            *both((NS, 2, 2)),
            *both((NS, 2, 2)),
            *both((NS, 2)),
            *both((NS, 2, 2)),
            *both((NS, 2, 2)),
            *both((NS, 3)),
            *both((NS,)),
            *both((1,)),
            *both((3,)),
            *both((3,)),
        ],
        compiler_params=pltpu.CompilerParams(
            collective_id=1, has_side_effects=True, vmem_limit_bytes=62 * 1024 * 1024
        ),
        cost_estimate=pl.CostEstimate(
            flops=20_000_000_000, bytes_accessed=3_000_000, transcendentals=0
        ),
    )(rotation, gradient)
    return updated, norms.reshape(256)


def solution(mesh):
    placed = (P("row", "col"), P("row", "col"))
    return jax.shard_map(
        on_device,
        mesh=mesh,
        in_specs=placed,
        out_specs=(P("row", "col"), P("col")),
        check_vma=False,
    )
```

```python
import jax
import jax.numpy as jnp
from jax import lax
from jax.experimental import pallas as pl
from jax.experimental.pallas import tpu as pltpu
from jax.sharding import PartitionSpec as P

MESH = pl.DeviceIdType.MESH
F32 = jnp.float32
BF16 = jnp.bfloat16
NS = 8
CH = 16
BLK = 1024
HALF = 512
TILE = 512
ITEMS = 2 * NS


def step_kernel(
    rot_hbm, grad_hbm, out_ref, norm_ref,
    rot, grad, base, base_out, panel, part, full, mine, ring_a, ring_b, swapped,
    term, term_in, kept, tail, tail_in, upd, turned, turned_in, sq, sq_y, sq_sum, sq_in,
    load_sem, pair_s, pair_r, v0_s, v0_r, v1_s, v1_r, a_s, a_r, b_s, b_r, z_s, z_r,
    c_s, c_r, e_s, e_r, t_s, t_r, w_s, w_r, u_s, u_r, n_s, n_r, m_s, m_r,
):
    row = lax.axis_index("row")
    col = lax.axis_index("col")
    core, y, zh = row % 2, (row // 2) % 4, row // 8
    x, zl = col // 2, col % 2
    up, across, down = (y + 1) % 4, (y + 2) % 4, (y + 3) % 4

    def at_row(zh_, y_, core_):
        return {"row": zh_ * 8 + y_ * 2 + core_, "col": col}

    def at_col(x_, zl_):
        return {"row": row, "col": x_ * 2 + zl_}

    pair = at_row(zh, y, 1 - core)
    y_dev = (at_row(zh, up, core), at_row(zh, down, core))
    y_q = (up, down)
    y_all = tuple(at_row(zh, (y + k) % 4, core) for k in (1, 2, 3))
    z_dev = at_row(1 - zh, y, core)
    zc_dev = at_row(1 - zh, y, 1 - core)
    x_all = tuple(at_col((x + k) % 4, zl) for k in (1, 2, 3))
    zl_dev = at_col(x, 1 - zl)

    def send(src, dst, s, r, dev):
        return pltpu.make_async_remote_copy(
            src_ref=src, dst_ref=dst, send_sem=s, recv_sem=r, device_id=dev, device_id_type=MESH
        )

    own_rows = pl.ds(pl.multiple_of(core * HALF, HALF), HALF)
    other_rows = pl.ds(pl.multiple_of((1 - core) * HALF, HALF), HALF)
    loads = [
        pltpu.make_async_copy(rot_hbm, rot.at[own_rows], load_sem.at[0]),
        pltpu.make_async_copy(grad_hbm, grad.at[own_rows], load_sem.at[1]),
    ]
    for c in loads:
        c.start()

    barrier = pltpu.get_barrier_semaphore()
    peers = (pair, *y_all, z_dev, zc_dev, *x_all, zl_dev)
    for dev in peers:
        pl.semaphore_signal(barrier, inc=1, device_id=dev, device_id_type=MESH)

    pick = lax.broadcasted_iota(jnp.int32, (128, HALF), 1) == 4 * lax.broadcasted_iota(
        jnp.int32, (128, HALF), 0
    )
    pick = pick.astype(F32).astype(BF16)

    def picked(side):
        cols = pl.ds(pl.multiple_of(side * HALF, HALF), HALF)
        return (
            lax.dot_general(
                pick, rot[own_rows, cols], (((1,), (1,)), ((), ())), preferred_element_type=F32
            )
            .astype(BF16)
            .reshape(NS, CH, HALF)
        )

    loads[0].wait()
    base_out[...] = picked(1 - core)
    base[:, :, own_rows] = picked(core)
    loads[1].wait()

    pl.semaphore_wait(barrier, len(peers))
    pairs = [
        send(base_out, base.at[:, :, own_rows], pair_s.at[0], pair_r.at[0], pair),
        send(rot.at[own_rows], rot.at[own_rows], pair_s.at[1], pair_r.at[1], pair),
        send(grad.at[own_rows], grad.at[own_rows], pair_s.at[2], pair_r.at[2], pair),
    ]
    for c in pairs:
        c.start()
    pairs[0].wait_recv()

    def v0(i):
        k = i % NS
        return send(panel.at[k, x, zl], panel.at[k, x, zl], v0_s.at[k], v0_r.at[k], zl_dev)

    def v1(i, d):
        k = i % NS
        return send(panel.at[k, x], panel.at[k, x], v1_s.at[k, d], v1_r.at[k, d], x_all[d])

    def ra(i, h, d):
        k = i % NS
        return send(
            part.at[k, h, across, d], ring_a.at[k, h, d], a_s.at[k, h, d], a_r.at[k, h, d], y_dev[d]
        )

    def rb(i, h, d):
        k = i % NS
        return send(
            part.at[k, h, y_q[d]], ring_b.at[k, h, d], b_s.at[k, h, d], b_r.at[k, h, d], y_dev[d]
        )

    def zx(i, h):
        k = i % NS
        return send(mine.at[k, h], swapped.at[k, h], z_s.at[k, h], z_r.at[k, h], z_dev)

    def ga(i, h, d):
        k = i % NS
        return send(
            full.at[k, h, y], full.at[k, h, y], c_s.at[k, h, d], c_r.at[k, h, d], y_dev[d]
        )

    def gb(i, h, d):
        k = i % NS
        q = y_q[1 - d]
        return send(
            full.at[k, h, q, d], full.at[k, h, q, d], e_s.at[k, h, d], e_r.at[k, h, d], y_dev[d]
        )

    def tx(i, d):
        k = i % NS
        return send(
            term.at[k, (x + d + 1) % 4], term_in.at[k, d], t_s.at[k, d], t_r.at[k, d], x_all[d]
        )

    def wz(i):
        k = i % NS
        return send(tail.at[k], tail_in.at[k], w_s.at[k], w_r.at[k], zl_dev)

    for j in range(NS):
        panel[j, x, zl] = base[j]
    for j in range(NS):
        v0(j).start()
    for j in range(NS):
        v0(j).wait_recv()
        for d in range(3):
            v1(j, d).start()
    pairs[1].wait_recv()
    pairs[2].wait_recv()

    def project(i, h):
        k = i % NS
        held = (rot, grad)[h]
        lhs = panel[k].reshape(8 * CH, BLK)

        @pl.loop(0, BLK // TILE)
        def _(n):
            cols = pl.ds(pl.multiple_of(n * TILE, TILE), TILE)
            z = jnp.dot(lhs, held[:, cols], preferred_element_type=F32)
            part[k, h, :, :, :, cols] = z.astype(BF16).reshape(4, 2, CH, TILE)

    def apply(i):
        k = i % NS

        @pl.loop(0, BLK // TILE)
        def _(n):
            rows = pl.ds(pl.multiple_of(n * TILE, TILE), TILE)
            nt = (((1,), (1,)), ((), ()))
            t = lax.dot_general(
                full[k, 0].reshape(8 * CH, BLK), grad[rows, :], nt, preferred_element_type=F32
            ) - lax.dot_general(
                full[k, 1].reshape(8 * CH, BLK), rot[rows, :], nt, preferred_element_type=F32
            )
            term[k, :, :, :, rows] = t.astype(BF16).reshape(4, 2, CH, TILE)

    every = [(h, d) for h in range(2) for d in range(2)]

    def run(i, _):
        def stage(late):
            return pl.when((i >= late) & (i < ITEMS + late))

        @stage(5)
        def _():
            it = i - 5
            for h in range(2):
                for d in range(2):
                    ga(it, h, d).wait_recv()
                for d in range(2):
                    gb(it, h, d).start()
            for h in range(2):
                zx(it, h).wait_send()

        @stage(4)
        def _():
            it = i - 4
            k = it % NS
            for h in range(2):
                zx(it, h).wait_recv()
                z = mine[k, h].astype(F32) + swapped[k, h].astype(F32)
                full[k, h, y] = z.astype(BF16)
                for d in range(2):
                    ga(it, h, d).start()
            for h, d in every:
                rb(it, h, d).wait_send()

        @stage(3)
        def _():
            it = i - 3
            k = it % NS
            for h in range(2):
                for d in range(2):
                    rb(it, h, d).wait_recv()
                s = part[k, h, y].astype(F32) + (
                    ring_b[k, h, 0].astype(F32) + ring_b[k, h, 1].astype(F32)
                )
                mine[k, h] = s.astype(BF16)
                zx(it, h).start()
            for h, d in every:
                ra(it, h, d).wait_send()

        @stage(8)
        def _():
            it = i - 8
            k = it % NS
            wz(it).wait_recv()
            applied = kept[k] + tail_in[k].astype(F32)
            b = base[k].astype(F32)

            @pl.when(i < ITEMS)
            def _():
                first = b + 0.25 * applied
                panel[k, x, zl] = (b + first).astype(BF16)
                v0(i).start()

            @pl.when(i >= ITEMS)
            def _():
                upd[k] = b + 0.125 * applied

            for d in range(3):
                tx(it, d).wait_send()
            wz(it).wait_send()

        @stage(2)
        def _():
            it = i - 2
            k = it % NS
            for h, d in every:
                ra(it, h, d).wait_recv()
                total = part[k, h, y_q[d], d].astype(F32) + ring_a[k, h, d].astype(F32)
                part[k, h, y_q[d], d] = total.astype(BF16)
                rb(it, h, d).start()
            for d in range(3):
                v1(it, d).wait_send()

        @stage(6)
        def _():
            it = i - 6
            for h, d in every:
                gb(it, h, d).wait_recv()
            apply(it)
            for d in range(3):
                tx(it, d).start()
            for h, d in every:
                ga(it, h, d).wait_send()

        @pl.when((i >= NS) & (i < ITEMS))
        def _():
            v0(i).wait_recv()
            for d in range(3):
                v1(i, d).start()

        @stage(7)
        def _():
            it = i - 7
            k = it % NS
            for d in range(3):
                tx(it, d).wait_recv()

            def summed(z):
                return (term[k, x, z].astype(F32) + term_in[k, 0, z].astype(F32)) + (
                    term_in[k, 1, z].astype(F32) + term_in[k, 2, z].astype(F32)
                )

            tail[k] = summed(1 - zl).astype(BF16)
            wz(it).start()
            kept[k] = summed(zl)
            for h, d in every:
                gb(it, h, d).wait_send()

        @stage(1)
        def _():
            it = i - 1
            for d in range(3):
                v1(it, d).wait_recv()
            for h in range(2):
                project(it, h)
                for d in range(2):
                    ra(it, h, d).start()
            v0(it).wait_send()

        return 0

    lax.fori_loop(1, ITEMS + 8, run, 0)

    total = jnp.zeros((1, 128), F32)
    for r in range(BLK // 128):
        block = upd[:, :, r * 128 : (r + 1) * 128].reshape(128, 128).T
        turned[r * 128 : (r + 1) * 128, :] = block
        total = total + jnp.sum(block * block, axis=0, keepdims=True)
    sq[...] = jnp.broadcast_to(total, (8, 128))
    swap = send(turned.at[other_rows], turned_in, u_s.at[0], u_r.at[0], pair)
    swap.start()
    ys = [send(sq, sq_y.at[k], n_s.at[k], n_r.at[k], y_all[k]) for k in range(3)]
    for c in ys:
        c.start()
    out_ref[:, pl.ds(pl.multiple_of(core * 128, 128), 128)] = turned[own_rows, :]
    for c in ys:
        c.wait_recv()
    sq_sum[...] = (sq[...] + sq_y[0]) + (sq_y[1] + sq_y[2])
    ms = [
        send(sq_sum, sq_in.at[k], m_s.at[k], m_r.at[k], dev)
        for k, dev in enumerate((z_dev, pair, zc_dev))
    ]
    for c in ms:
        c.start()
    swap.wait_recv()
    out_ref[:, pl.ds(pl.multiple_of((1 - core) * 128, 128), 128)] = turned_in[...]
    for c in ms:
        c.wait_recv()
    own_norm = jnp.sqrt(sq_sum[0:1, :] + sq_in[0, 0:1, :])
    other_norm = jnp.sqrt(sq_in[1, 0:1, :] + sq_in[2, 0:1, :])
    norm_ref[0:1, :] = jnp.where(core == 0, own_norm, other_norm)
    norm_ref[1:2, :] = jnp.where(core == 0, other_norm, own_norm)
    for c in (*pairs, swap, *ys, *ms):
        c.wait_send()


def on_device(rotation, gradient):
    dma = pltpu.SemaphoreType.DMA

    def both(shape):
        return [dma(shape), dma(shape)]

    quarters = (4, 2, CH, BLK)
    updated, norms = pl.pallas_call(
        step_kernel,
        name="cayley_step",
        out_shape=(
            jax.ShapeDtypeStruct((HALF, 256), F32),
            jax.ShapeDtypeStruct((2, 128), F32),
        ),
        in_specs=[pl.BlockSpec(memory_space=pl.ANY)] * 2,
        out_specs=(
            pl.BlockSpec(memory_space=pltpu.VMEM),
            pl.BlockSpec(memory_space=pltpu.VMEM),
        ),
        scratch_shapes=[
            pltpu.VMEM((BLK, BLK), BF16),
            pltpu.VMEM((BLK, BLK), BF16),
            pltpu.VMEM((NS, CH, BLK), BF16),
            pltpu.VMEM((NS, CH, HALF), BF16),
            pltpu.VMEM((NS, *quarters), BF16),
            pltpu.VMEM((NS, 2, *quarters), BF16),
            pltpu.VMEM((NS, 2, *quarters), BF16),
            pltpu.VMEM((NS, 2, 2, CH, BLK), BF16),
            pltpu.VMEM((NS, 2, 2, CH, BLK), BF16),
            pltpu.VMEM((NS, 2, 2, 2, CH, BLK), BF16),
            pltpu.VMEM((NS, 2, 2, CH, BLK), BF16),
            pltpu.VMEM((NS, *quarters), BF16),
            pltpu.VMEM((NS, 3, 2, CH, BLK), BF16),
            pltpu.VMEM((NS, CH, BLK), F32),
            pltpu.VMEM((NS, CH, BLK), BF16),
            pltpu.VMEM((NS, CH, BLK), BF16),
            pltpu.VMEM((NS, CH, BLK), F32),
            pltpu.VMEM((BLK, 128), F32),
            pltpu.VMEM((HALF, 128), F32),
            pltpu.VMEM((8, 128), F32),
            pltpu.VMEM((3, 8, 128), F32),
            pltpu.VMEM((8, 128), F32),
            pltpu.VMEM((3, 8, 128), F32),
            dma((2,)),
            *both((3,)),
            *both((NS,)),
            *both((NS, 3)),
            *both((NS, 2, 2)),
            *both((NS, 2, 2)),
            *both((NS, 2)),
            *both((NS, 2, 2)),
            *both((NS, 2, 2)),
            *both((NS, 3)),
            *both((NS,)),
            *both((1,)),
            *both((3,)),
            *both((3,)),
        ],
        compiler_params=pltpu.CompilerParams(
            collective_id=1, has_side_effects=True, vmem_limit_bytes=62 * 1024 * 1024
        ),
        cost_estimate=pl.CostEstimate(
            flops=20_000_000_000, bytes_accessed=3_000_000, transcendentals=0
        ),
    )(rotation, gradient)
    return updated, norms.reshape(256)


def solution(mesh):
    placed = (P("row", "col"), P("row", "col"))
    return jax.shard_map(
        on_device,
        mesh=mesh,
        in_specs=placed,
        out_specs=(P("row", "col"), P("col")),
        check_vma=False,
    )
```

```python
import jax
import jax.numpy as jnp
from jax import lax
from jax.experimental import pallas as pl
from jax.experimental.pallas import tpu as pltpu
from jax.sharding import PartitionSpec as P

MESH = pl.DeviceIdType.MESH
F32 = jnp.float32
BF16 = jnp.bfloat16
NS = 8
CH = 16
BLK = 1024
HALF = 512
TILE = 512
ITEMS = 2 * NS
CUT = 384
WIDE = (BLK, CUT)


def step_kernel(
    rot_hbm, grad_hbm, out_ref, norm_ref,
    rot, grad, base, base_out, panel, part, full, mine, ring_a, ring_b, swapped, far, far_in, far_y,
    term, term_in, kept, tail, tail_in, upd, turned, turned_in, sq, sq_y, sq_sum, sq_in,
    load_sem, pair_s, pair_r, v0_s, v0_r, v1_s, v1_r, a_s, a_r, b_s, b_r, z_s, z_r,
    c_s, c_r, e_s, e_r, fa_s, fa_r, fb_s, fb_r, fc_s, fc_r, fd_s, fd_r, t_s, t_r, w_s, w_r, u_s, u_r, n_s, n_r, m_s, m_r,
):
    row = lax.axis_index("row")
    col = lax.axis_index("col")
    core, y, zh = row % 2, (row // 2) % 4, row // 8
    x, zl = col // 2, col % 2
    up, across, down = (y + 1) % 4, (y + 2) % 4, (y + 3) % 4

    def at_row(zh_, y_, core_):
        return {"row": zh_ * 8 + y_ * 2 + core_, "col": col}

    def at_col(x_, zl_):
        return {"row": row, "col": x_ * 2 + zl_}

    pair = at_row(zh, y, 1 - core)
    y_dev = (at_row(zh, up, core), at_row(zh, down, core))
    y_q = (up, down)
    y_all = tuple(at_row(zh, (y + k) % 4, core) for k in (1, 2, 3))
    z_dev = at_row(1 - zh, y, core)
    zc_dev = at_row(1 - zh, y, 1 - core)
    x_all = tuple(at_col((x + k) % 4, zl) for k in (1, 2, 3))
    zl_dev = at_col(x, 1 - zl)

    def send(src, dst, s, r, dev):
        return pltpu.make_async_remote_copy(
            src_ref=src, dst_ref=dst, send_sem=s, recv_sem=r, device_id=dev, device_id_type=MESH
        )

    own_rows = pl.ds(pl.multiple_of(core * HALF, HALF), HALF)
    other_rows = pl.ds(pl.multiple_of((1 - core) * HALF, HALF), HALF)
    loads = [
        pltpu.make_async_copy(rot_hbm, rot.at[own_rows], load_sem.at[0]),
        pltpu.make_async_copy(grad_hbm, grad.at[own_rows], load_sem.at[1]),
    ]
    for c in loads:
        c.start()

    barrier = pltpu.get_barrier_semaphore()
    peers = (pair, *y_all, z_dev, zc_dev, *x_all, zl_dev)
    for dev in peers:
        pl.semaphore_signal(barrier, inc=1, device_id=dev, device_id_type=MESH)

    pick = lax.broadcasted_iota(jnp.int32, (128, HALF), 1) == 4 * lax.broadcasted_iota(
        jnp.int32, (128, HALF), 0
    )
    pick = pick.astype(F32).astype(BF16)

    def picked(side):
        cols = pl.ds(pl.multiple_of(side * HALF, HALF), HALF)
        return (
            lax.dot_general(
                pick, rot[own_rows, cols], (((1,), (1,)), ((), ())), preferred_element_type=F32
            )
            .astype(BF16)
            .reshape(NS, CH, HALF)
        )

    loads[0].wait()
    base_out[...] = picked(1 - core)
    base[:, :, own_rows] = picked(core)
    loads[1].wait()

    pl.semaphore_wait(barrier, len(peers))
    pairs = [
        send(base_out, base.at[:, :, own_rows], pair_s.at[0], pair_r.at[0], pair),
        send(rot.at[own_rows], rot.at[own_rows], pair_s.at[1], pair_r.at[1], pair),
        send(grad.at[own_rows], grad.at[own_rows], pair_s.at[2], pair_r.at[2], pair),
    ]
    for c in pairs:
        c.start()
    pairs[0].wait_recv()

    def v0(i):
        k = i % NS
        return send(panel.at[k, x, zl], panel.at[k, x, zl], v0_s.at[k], v0_r.at[k], zl_dev)

    def v1(i, d):
        k = i % NS
        return send(panel.at[k, x], panel.at[k, x], v1_s.at[k, d], v1_r.at[k, d], x_all[d])

    def first(h):
        return pl.ds(0, WIDE[h])

    def ra(i, h, d):
        k = i % NS
        return send(
            part.at[k, h, across, d, :, first(h)],
            ring_a.at[k, h, d, :, first(h)],
            a_s.at[k, h, d],
            a_r.at[k, h, d],
            y_dev[d],
        )

    def rb(i, h, d):
        k = i % NS
        return send(
            part.at[k, h, y_q[d], :, :, first(h)],
            ring_b.at[k, h, d, :, :, first(h)],
            b_s.at[k, h, d],
            b_r.at[k, h, d],
            y_dev[d],
        )

    def zx(i, h):
        k = i % NS
        return send(
            mine.at[k, h, :, :, first(h)], swapped.at[k, h, :, :, first(h)], z_s.at[k, h], z_r.at[k, h], z_dev
        )

    def ga(i, h, d):
        k = i % NS
        return send(
            full.at[k, h, y, :, :, first(h)],
            full.at[k, h, y, :, :, first(h)],
            c_s.at[k, h, d],
            c_r.at[k, h, d],
            y_dev[d],
        )

    def gb(i, h, d):
        k = i % NS
        q = y_q[1 - d]
        return send(
            full.at[k, h, q, d, :, first(h)],
            full.at[k, h, q, d, :, first(h)],
            e_s.at[k, h, d],
            e_r.at[k, h, d],
            y_dev[d],
        )

    rest = pl.ds(CUT, BLK - CUT)

    def fa(i):
        k = i % NS
        return send(
            part.at[k, 1, :, 1 - zh, :, rest], far_in.at[k], fa_s.at[k], fa_r.at[k], z_dev
        )

    def fb(i, d):
        k = i % NS
        return send(
            far.at[k, (y + d + 1) % 4], far_y.at[k, d], fb_s.at[k, d], fb_r.at[k, d], y_all[d]
        )

    def fc(i, d):
        k = i % NS
        place = full.at[k, 1, y, zh, :, rest]
        return send(place, place, fc_s.at[k, d], fc_r.at[k, d], y_all[d])

    def fd(i):
        k = i % NS
        place = full.at[k, 1, :, zh, :, rest]
        return send(place, place, fd_s.at[k], fd_r.at[k], z_dev)

    def tx(i, d):
        k = i % NS
        return send(
            term.at[k, (x + d + 1) % 4], term_in.at[k, d], t_s.at[k, d], t_r.at[k, d], x_all[d]
        )

    def wz(i):
        k = i % NS
        return send(tail.at[k], tail_in.at[k], w_s.at[k], w_r.at[k], zl_dev)

    for j in range(NS):
        panel[j, x, zl] = base[j]
    for j in range(NS):
        v0(j).start()
    for j in range(NS):
        v0(j).wait_recv()
        for d in range(3):
            v1(j, d).start()
    pairs[1].wait_recv()
    pairs[2].wait_recv()

    def project(i, h):
        k = i % NS
        held = (rot, grad)[h]
        lhs = panel[k].reshape(8 * CH, BLK)

        @pl.loop(0, BLK // TILE)
        def _(n):
            cols = pl.ds(pl.multiple_of(n * TILE, TILE), TILE)
            z = jnp.dot(lhs, held[:, cols], preferred_element_type=F32)
            part[k, h, :, :, :, cols] = z.astype(BF16).reshape(4, 2, CH, TILE)

    def apply(i):
        k = i % NS

        @pl.loop(0, BLK // TILE)
        def _(n):
            rows = pl.ds(pl.multiple_of(n * TILE, TILE), TILE)
            nt = (((1,), (1,)), ((), ()))
            t = lax.dot_general(
                full[k, 0].reshape(8 * CH, BLK), grad[rows, :], nt, preferred_element_type=F32
            ) - lax.dot_general(
                full[k, 1].reshape(8 * CH, BLK), rot[rows, :], nt, preferred_element_type=F32
            )
            term[k, :, :, :, rows] = t.astype(BF16).reshape(4, 2, CH, TILE)

    every = [(h, d) for h in range(2) for d in range(2)]

    def run(i, _):
        def stage(late):
            return pl.when((i >= late) & (i < ITEMS + late))

        @pl.when((i > NS) & (i <= ITEMS))
        def _():
            v0(i - 1).wait_recv()
            for d in range(3):
                v1(i - 1, d).start()

        @stage(5)
        def _():
            it = i - 5
            for h in range(2):
                for d in range(2):
                    ga(it, h, d).wait_recv()
                for d in range(2):
                    gb(it, h, d).start()
            for h in range(2):
                zx(it, h).wait_send()
            for d in range(3):
                fc(it, d).wait_send()

        @stage(4)
        def _():
            it = i - 4
            k = it % NS
            for h in range(2):
                zx(it, h).wait_recv()
                w = first(h)
                z = mine[k, h, :, :, w].astype(F32) + swapped[k, h, :, :, w].astype(F32)
                full[k, h, y, :, :, w] = z.astype(BF16)
                for d in range(2):
                    ga(it, h, d).start()
            for h, d in every:
                rb(it, h, d).wait_send()
            for d in range(3):
                fb(it, d).wait_send()

        @stage(3)
        def _():
            it = i - 3
            k = it % NS
            for h in range(2):
                for d in range(2):
                    rb(it, h, d).wait_recv()
                w = first(h)
                s = part[k, h, y, :, :, w].astype(F32) + (
                    ring_b[k, h, 0, :, :, w].astype(F32) + ring_b[k, h, 1, :, :, w].astype(F32)
                )
                mine[k, h, :, :, w] = s.astype(BF16)
                zx(it, h).start()
            for d in range(3):
                fb(it, d).wait_recv()
            s = (far[k, y].astype(F32) + far_y[k, 0].astype(F32)) + (
                far_y[k, 1].astype(F32) + far_y[k, 2].astype(F32)
            )
            full[k, 1, y, zh, :, rest] = s.astype(BF16)
            for d in range(3):
                fc(it, d).start()
            for h, d in every:
                ra(it, h, d).wait_send()
            fa(it).wait_send()

        @stage(8)
        def _():
            it = i - 8
            k = it % NS
            wz(it).wait_recv()
            applied = kept[k] + tail_in[k].astype(F32)
            b = base[k].astype(F32)

            @pl.when(i < ITEMS)
            def _():
                first = b + 0.25 * applied
                panel[k, x, zl] = (b + first).astype(BF16)
                v0(i).start()

            @pl.when(i >= ITEMS)
            def _():
                upd[k] = b + 0.125 * applied

            for d in range(3):
                tx(it, d).wait_send()
            wz(it).wait_send()

        @stage(4)
        def _():
            it = i - 4
            for d in range(3):
                fc(it, d).wait_recv()
            fd(it).start()

        @stage(2)
        def _():
            it = i - 2
            k = it % NS
            for h, d in every:
                ra(it, h, d).wait_recv()
                w = first(h)
                total = part[k, h, y_q[d], d, :, w].astype(F32) + ring_a[k, h, d, :, w].astype(F32)
                part[k, h, y_q[d], d, :, w] = total.astype(BF16)
                rb(it, h, d).start()
            fa(it).wait_recv()
            sums = part[k, 1, :, zh, :, rest].astype(F32) + far_in[k].astype(F32)
            far[k] = sums.astype(BF16)
            for d in range(3):
                fb(it, d).start()
            for d in range(3):
                v1(it, d).wait_send()

        @stage(6)
        def _():
            it = i - 6
            for h, d in every:
                gb(it, h, d).wait_recv()
            fd(it).wait_recv()
            apply(it)
            for d in range(3):
                tx(it, d).start()
            for h, d in every:
                ga(it, h, d).wait_send()
            fd(it).wait_send()

        @stage(7)
        def _():
            it = i - 7
            k = it % NS
            for d in range(3):
                tx(it, d).wait_recv()

            def summed(z):
                return (term[k, x, z].astype(F32) + term_in[k, 0, z].astype(F32)) + (
                    term_in[k, 1, z].astype(F32) + term_in[k, 2, z].astype(F32)
                )

            tail[k] = summed(1 - zl).astype(BF16)
            wz(it).start()
            kept[k] = summed(zl)
            for h, d in every:
                gb(it, h, d).wait_send()

        @stage(1)
        def _():
            it = i - 1
            for d in range(3):
                v1(it, d).wait_recv()
            for h in range(2):
                project(it, 1 - h)
                if h == 0:
                    fa(it).start()
                for d in range(2):
                    ra(it, 1 - h, d).start()
            v0(it).wait_send()

        return 0

    lax.fori_loop(1, ITEMS + 8, run, 0)

    total = jnp.zeros((1, 128), F32)
    for r in range(BLK // 128):
        block = upd[:, :, r * 128 : (r + 1) * 128].reshape(128, 128).T
        turned[r * 128 : (r + 1) * 128, :] = block
        total = total + jnp.sum(block * block, axis=0, keepdims=True)
    sq[...] = jnp.broadcast_to(total, (8, 128))
    swap = send(turned.at[other_rows], turned_in, u_s.at[0], u_r.at[0], pair)
    swap.start()
    ys = [send(sq, sq_y.at[k], n_s.at[k], n_r.at[k], y_all[k]) for k in range(3)]
    for c in ys:
        c.start()
    out_ref[:, pl.ds(pl.multiple_of(core * 128, 128), 128)] = turned[own_rows, :]
    for c in ys:
        c.wait_recv()
    sq_sum[...] = (sq[...] + sq_y[0]) + (sq_y[1] + sq_y[2])
    ms = [
        send(sq_sum, sq_in.at[k], m_s.at[k], m_r.at[k], dev)
        for k, dev in enumerate((z_dev, pair, zc_dev))
    ]
    for c in ms:
        c.start()
    swap.wait_recv()
    out_ref[:, pl.ds(pl.multiple_of((1 - core) * 128, 128), 128)] = turned_in[...]
    for c in ms:
        c.wait_recv()
    own_norm = jnp.sqrt(sq_sum[0:1, :] + sq_in[0, 0:1, :])
    other_norm = jnp.sqrt(sq_in[1, 0:1, :] + sq_in[2, 0:1, :])
    norm_ref[0:1, :] = jnp.where(core == 0, own_norm, other_norm)
    norm_ref[1:2, :] = jnp.where(core == 0, other_norm, own_norm)
    for c in (*pairs, swap, *ys, *ms):
        c.wait_send()


def on_device(rotation, gradient):
    dma = pltpu.SemaphoreType.DMA

    def both(shape):
        return [dma(shape), dma(shape)]

    quarters = (4, 2, CH, BLK)
    updated, norms = pl.pallas_call(
        step_kernel,
        name="cayley_step",
        out_shape=(
            jax.ShapeDtypeStruct((HALF, 256), F32),
            jax.ShapeDtypeStruct((2, 128), F32),
        ),
        in_specs=[pl.BlockSpec(memory_space=pl.ANY)] * 2,
        out_specs=(
            pl.BlockSpec(memory_space=pltpu.VMEM),
            pl.BlockSpec(memory_space=pltpu.VMEM),
        ),
        scratch_shapes=[
            pltpu.VMEM((BLK, BLK), BF16),
            pltpu.VMEM((BLK, BLK), BF16),
            pltpu.VMEM((NS, CH, BLK), BF16),
            pltpu.VMEM((NS, CH, HALF), BF16),
            pltpu.VMEM((NS, *quarters), BF16),
            pltpu.VMEM((NS, 2, *quarters), BF16),
            pltpu.VMEM((NS, 2, *quarters), BF16),
            pltpu.VMEM((NS, 2, 2, CH, BLK), BF16),
            pltpu.VMEM((NS, 2, 2, CH, BLK), BF16),
            pltpu.VMEM((NS, 2, 2, 2, CH, BLK), BF16),
            pltpu.VMEM((NS, 2, 2, CH, BLK), BF16),
            pltpu.VMEM((NS, 4, CH, BLK - CUT), BF16),
            pltpu.VMEM((NS, 4, CH, BLK - CUT), BF16),
            pltpu.VMEM((NS, 3, CH, BLK - CUT), BF16),
            pltpu.VMEM((NS, *quarters), BF16),
            pltpu.VMEM((NS, 3, 2, CH, BLK), BF16),
            pltpu.VMEM((NS, CH, BLK), F32),
            pltpu.VMEM((NS, CH, BLK), BF16),
            pltpu.VMEM((NS, CH, BLK), BF16),
            pltpu.VMEM((NS, CH, BLK), F32),
            pltpu.VMEM((BLK, 128), F32),
            pltpu.VMEM((HALF, 128), F32),
            pltpu.VMEM((8, 128), F32),
            pltpu.VMEM((3, 8, 128), F32),
            pltpu.VMEM((8, 128), F32),
            pltpu.VMEM((3, 8, 128), F32),
            dma((2,)),
            *both((3,)),
            *both((NS,)),
            *both((NS, 3)),
            *both((NS, 2, 2)),
            *both((NS, 2, 2)),
            *both((NS, 2)),
            *both((NS, 2, 2)),
            *both((NS, 2, 2)),
            *both((NS,)),
            *both((NS, 3)),
            *both((NS, 3)),
            *both((NS,)),
            *both((NS, 3)),
            *both((NS,)),
            *both((1,)),
            *both((3,)),
            *both((3,)),
        ],
        compiler_params=pltpu.CompilerParams(
            collective_id=1, has_side_effects=True, vmem_limit_bytes=62 * 1024 * 1024
        ),
        cost_estimate=pl.CostEstimate(
            flops=20_000_000_000, bytes_accessed=3_000_000, transcendentals=0
        ),
    )(rotation, gradient)
    return updated, norms.reshape(256)


def solution(mesh):
    placed = (P("row", "col"), P("row", "col"))
    return jax.shard_map(
        on_device,
        mesh=mesh,
        in_specs=placed,
        out_specs=(P("row", "col"), P("col")),
        check_vma=False,
    )
```

```python
import jax
import jax.numpy as jnp
from jax import lax
from jax.experimental import pallas as pl
from jax.experimental.pallas import tpu as pltpu
from jax.sharding import PartitionSpec as P

MESH = pl.DeviceIdType.MESH
F32 = jnp.float32
BF16 = jnp.bfloat16
NS = 8
CH = 16
BLK = 1024
HALF = 512
TILE = 512
ITEMS = 2 * NS
NQ = 2
NL = 4
CUT = 384
WIDE = (BLK, CUT)
EARLY = 0
LATE = ITEMS - 1


def step_kernel(
    rot_hbm, grad_hbm, out_ref, norm_ref,
    rot, grad, base, base_out, panel, part, full, mine, ring_a, ring_b, swapped, far, far_in, far_y,
    term, term_in, kept, tail, tail_in, upd, squares, turned, turned_in, sq, sq_y, sq_sum, sq_in,
    load_sem, pair_s, pair_r, v0_s, v0_r, v1_s, v1_r, a_s, a_r, b_s, b_r, z_s, z_r,
    c_s, c_r, e_s, e_r, fa_s, fa_r, fb_s, fb_r, fc_s, fc_r, fd_s, fd_r, t_s, t_r, w_s, w_r, u_s, u_r, n_s, n_r, m_s, m_r,
):
    row = lax.axis_index("row")
    col = lax.axis_index("col")
    core, y, zh = row % 2, (row // 2) % 4, row // 8
    x, zl = col // 2, col % 2
    up, across, down = (y + 1) % 4, (y + 2) % 4, (y + 3) % 4

    def at_row(zh_, y_, core_):
        return {"row": zh_ * 8 + y_ * 2 + core_, "col": col}

    def at_col(x_, zl_):
        return {"row": row, "col": x_ * 2 + zl_}

    pair = at_row(zh, y, 1 - core)
    y_dev = (at_row(zh, up, core), at_row(zh, down, core))
    y_q = (up, down)
    y_all = tuple(at_row(zh, (y + k) % 4, core) for k in (1, 2, 3))
    z_dev = at_row(1 - zh, y, core)
    zc_dev = at_row(1 - zh, y, 1 - core)
    x_all = tuple(at_col((x + k) % 4, zl) for k in (1, 2, 3))
    x_far = tuple(at_col((x + k) % 4, 1 - zl) for k in (1, 2, 3))
    zl_dev = at_col(x, 1 - zl)

    def send(src, dst, s, r, dev):
        return pltpu.make_async_remote_copy(
            src_ref=src, dst_ref=dst, send_sem=s, recv_sem=r, device_id=dev, device_id_type=MESH
        )

    own_rows = pl.ds(pl.multiple_of(core * HALF, HALF), HALF)
    other_rows = pl.ds(pl.multiple_of((1 - core) * HALF, HALF), HALF)
    loads = [
        pltpu.make_async_copy(rot_hbm, rot.at[own_rows], load_sem.at[0]),
        pltpu.make_async_copy(grad_hbm, grad.at[own_rows], load_sem.at[1]),
    ]
    for c in loads:
        c.start()

    barrier = pltpu.get_barrier_semaphore()
    peers = (pair, *y_all, z_dev, zc_dev, *x_all, *x_far, zl_dev)
    for dev in peers:
        pl.semaphore_signal(barrier, inc=1, device_id=dev, device_id_type=MESH)

    pick = lax.broadcasted_iota(jnp.int32, (128, HALF), 1) == 4 * lax.broadcasted_iota(
        jnp.int32, (128, HALF), 0
    )
    pick = pick.astype(F32).astype(BF16)

    def picked(side):
        cols = pl.ds(pl.multiple_of(side * HALF, HALF), HALF)
        return (
            lax.dot_general(
                pick, rot[own_rows, cols], (((1,), (1,)), ((), ())), preferred_element_type=F32
            )
            .astype(BF16)
            .reshape(NS, CH, HALF)
        )

    loads[0].wait()
    base_out[...] = picked(1 - core)
    base[:, :, own_rows] = picked(core)
    loads[1].wait()

    pl.semaphore_wait(barrier, len(peers))
    pairs = [
        send(base_out, base.at[:, :, own_rows], pair_s.at[0], pair_r.at[0], pair),
        send(rot.at[own_rows], rot.at[own_rows], pair_s.at[1], pair_r.at[1], pair),
        send(grad.at[own_rows], grad.at[own_rows], pair_s.at[2], pair_r.at[2], pair),
    ]
    for c in pairs:
        c.start()
    pairs[0].wait_recv()

    def first(h):
        return pl.ds(0, WIDE[h])

    rest = pl.ds(CUT, BLK - CUT)

    def v0(i):
        k = i % NS
        return send(panel.at[k, x, zl], panel.at[k, x, zl], v0_s.at[k], v0_r.at[k], zl_dev)

    def v1(i, d):
        k = i % NS
        return send(panel.at[k, x], panel.at[k, x], v1_s.at[k], v1_r.at[k], x_all[d])

    def v1_all(i):
        k = i % NS
        return send(term_in.at[k], term_in.at[k], v1_s.at[k], v1_r.at[k], zl_dev)

    def ra(i, h, d):
        k, q = i % NS, i % NQ
        return send(
            part.at[k, h, across, d, :, first(h)],
            ring_a.at[k, h, d, :, first(h)],
            a_s.at[q, h],
            a_r.at[q, h],
            y_dev[d],
        )

    def ra_all(i, h):
        k, q = i % NS, i % NQ
        ref = ring_a.at[k, h, :, :, first(h)]
        return send(ref, ref, a_s.at[q, h], a_r.at[q, h], zl_dev)

    def rb(i, h, d):
        k, q = i % NS, i % NQ
        return send(
            part.at[k, h, y_q[d], :, :, first(h)],
            ring_b.at[k, h, d, :, :, first(h)],
            b_s.at[q, h],
            b_r.at[q, h],
            y_dev[d],
        )

    def rb_all(i, h):
        k, q = i % NS, i % NQ
        ref = ring_b.at[k, h, :, :, :, first(h)]
        return send(ref, ref, b_s.at[q, h], b_r.at[q, h], zl_dev)

    def zx(i, h):
        k, q = i % NS, i % NQ
        return send(
            mine.at[k, h, :, :, first(h)],
            swapped.at[k, h, :, :, first(h)],
            z_s.at[q, h],
            z_r.at[q, h],
            z_dev,
        )

    def ga(i, h, d):
        k, q = i % NS, i % NL
        place = full.at[k, h, y, :, :, first(h)]
        return send(place, place, c_s.at[q, h], c_r.at[q, h], y_dev[d])

    def ga_all(i, h):
        k, q = i % NS, i % NL
        ref = ring_b.at[k, h, :, :, :, first(h)]
        return send(ref, ref, c_s.at[q, h], c_r.at[q, h], zl_dev)

    def gb(i, h, d):
        k, q = i % NS, i % NL
        place = full.at[k, h, y_q[1 - d], d, :, first(h)]
        return send(place, place, e_s.at[q, h], e_r.at[q, h], y_dev[d])

    def gb_all(i, h):
        k, q = i % NS, i % NL
        ref = ring_a.at[k, h, :, :, first(h)]
        return send(ref, ref, e_s.at[q, h], e_r.at[q, h], zl_dev)

    def fa(i):
        k, q = i % NS, i % NL
        return send(
            part.at[k, 1, :, 1 - zh, :, rest], far_in.at[k], fa_s.at[q], fa_r.at[q], z_dev
        )

    def fb(i, d):
        k, q = i % NS, i % NQ
        return send(
            far.at[k, (y + d + 1) % 4], far_y.at[k, d], fb_s.at[q], fb_r.at[q], y_all[d]
        )

    def fb_all(i):
        k, q = i % NS, i % NQ
        return send(far_y.at[k], far_y.at[k], fb_s.at[q], fb_r.at[q], zl_dev)

    def fc(i, d):
        k, q = i % NS, i % NQ
        place = full.at[k, 1, y, zh, :, rest]
        return send(place, place, fc_s.at[q], fc_r.at[q], y_all[d])

    def fc_all(i):
        k, q = i % NS, i % NQ
        return send(far_y.at[k], far_y.at[k], fc_s.at[q], fc_r.at[q], zl_dev)

    def fd(i):
        k, q = i % NS, i % NL
        place = full.at[k, 1, :, zh, :, rest]
        return send(place, place, fd_s.at[q], fd_r.at[q], z_dev)

    def tx(i, d):
        k, q = i % NS, i % NL
        return send(
            term.at[k, (x + d + 1) % 4], term_in.at[k, d], t_s.at[q], t_r.at[q], x_all[d]
        )

    def tx_all(i):
        k, q = i % NS, i % NL
        return send(term_in.at[k], term_in.at[k], t_s.at[q], t_r.at[q], zl_dev)

    def wz(i):
        k, q = i % NS, i % NL
        return send(tail.at[k], tail_in.at[k], w_s.at[q], w_r.at[q], zl_dev)

    for j in range(NS):
        panel[j, x, zl] = base[j]
    for j in range(EARLY):
        for d in range(3):
            place = panel.at[j, x, zl]
            for dev in (x_all[d], x_far[d]):
                send(place, place, v1_s.at[j], v1_r.at[j], dev).start()
    for j in range(NS):
        v0(j).start()
    for j in range(NS):
        v0(j).wait_recv()
        if j >= EARLY:
            for d in range(3):
                v1(j, d).start()
    pairs[1].wait_recv()
    pairs[2].wait_recv()

    def project(i, h):
        k = i % NS
        held = (rot, grad)[h]
        lhs = panel[k].reshape(8 * CH, BLK)

        @pl.loop(0, BLK // TILE)
        def _(n):
            cols = pl.ds(pl.multiple_of(n * TILE, TILE), TILE)
            z = jnp.dot(lhs, held[:, cols], preferred_element_type=F32)
            part[k, h, :, :, :, cols] = z.astype(BF16).reshape(4, 2, CH, TILE)

    def apply(i):
        k = i % NS

        @pl.loop(0, BLK // TILE)
        def _(n):
            rows = pl.ds(pl.multiple_of(n * TILE, TILE), TILE)
            nt = (((1,), (1,)), ((), ()))
            t = lax.dot_general(
                full[k, 0].reshape(8 * CH, BLK), grad[rows, :], nt, preferred_element_type=F32
            ) - lax.dot_general(
                full[k, 1].reshape(8 * CH, BLK), rot[rows, :], nt, preferred_element_type=F32
            )
            term[k, :, :, :, rows] = t.astype(BF16).reshape(4, 2, CH, TILE)

    def run(i, _):
        def stage(late):
            return pl.when((i >= late) & (i < ITEMS + late))

        @pl.when((i > NS) & (i <= ITEMS))
        def _():
            v0(i - 1).wait_recv()
            for d in range(3):
                v1(i - 1, d).start()

        @stage(5)
        def _():
            it = i - 5
            for h in range(2):
                ga_all(it, h).wait_recv()
                for d in range(2):
                    gb(it, h, d).start()
            for h in range(2):
                zx(it, h).wait_send()
            fc_all(it).wait_send()

        @stage(4)
        def _():
            it = i - 4
            k = it % NS
            for h in range(2):
                zx(it, h).wait_recv()
                w = first(h)
                z = mine[k, h, :, :, w].astype(F32) + swapped[k, h, :, :, w].astype(F32)
                full[k, h, y, :, :, w] = z.astype(BF16)
                for d in range(2):
                    ga(it, h, d).start()
            for h in range(2):
                rb_all(it, h).wait_send()

        @stage(3)
        def _():
            it = i - 3
            k = it % NS
            for h in range(2):
                rb_all(it, h).wait_recv()
                w = first(h)
                s = part[k, h, y, :, :, w].astype(F32) + (
                    ring_b[k, h, 0, :, :, w].astype(F32) + ring_b[k, h, 1, :, :, w].astype(F32)
                )
                mine[k, h, :, :, w] = s.astype(BF16)
                zx(it, h).start()
            for h in range(2):
                ra_all(it, h).wait_send()

        @stage(8)
        def _():
            it = i - 8
            k = it % NS
            wz(it).wait_recv()
            applied = kept[k] + tail_in[k].astype(F32)
            b = base[k].astype(F32)

            @pl.when(i < ITEMS)
            def _():
                first = b + 0.25 * applied
                panel[k, x, zl] = (b + first).astype(BF16)
                v0(i).start()

            @pl.when(i >= ITEMS)
            def _():
                new = b + 0.125 * applied
                upd[k] = new
                lanes = new[:, :128] * new[:, :128]
                for r in range(1, BLK // 128):
                    lane = new[:, r * 128 : (r + 1) * 128]
                    lanes = lanes + lane * lane
                squares[k] = lanes

            tx_all(it).wait_send()
            wz(it).wait_send()

        @stage(2)
        def _():
            it = i - 2
            k = it % NS
            for h in range(2):
                w = first(h)
                ra_all(it, h).wait_recv()
                for d in range(2):
                    there = part[k, h, y_q[d], d, :, w].astype(F32)
                    there = there + ring_a[k, h, d, :, w].astype(F32)
                    part[k, h, y_q[d], d, :, w] = there.astype(BF16)
                    rb(it, h, d).start()
            v1_all(it).wait_send()

        @stage(6)
        def _():
            it = i - 6
            for h in range(2):
                gb_all(it, h).wait_recv()
            fd(it).wait_recv()
            apply(it)
            k, q = it % NS, it % NL

            @pl.when(it < LATE)
            def _():
                for d in range(3):
                    tx(it, d).start()

            @pl.when(it >= LATE)
            def _():
                for d in range(3):
                    for z, dev in ((0, x_all[d]), (1, x_far[d])):
                        src = term.at[k, (x + d + 1) % 4, zl + z - 2 * zl * z]
                        send(src, term_in.at[k, d, z], t_s.at[q], t_r.at[q], dev).start()
                send(term.at[k, x, 1 - zl], tail_in.at[k], w_s.at[q], w_r.at[q], zl_dev).start()

            for h in range(2):
                ga_all(it, h).wait_send()
            fd(it).wait_send()

        @stage(7)
        def _():
            it = i - 7
            k = it % NS
            tx_all(it).wait_recv()

            def summed(z):
                return (term[k, x, z].astype(F32) + term_in[k, 0, z].astype(F32)) + (
                    term_in[k, 1, z].astype(F32) + term_in[k, 2, z].astype(F32)
                )

            @pl.when(it < LATE)
            def _():
                tail[k] = summed(1 - zl).astype(BF16)
                wz(it).start()
                kept[k] = summed(zl)

            @pl.when(it >= LATE)
            def _():
                total = term[k, x, zl].astype(F32)
                for d in range(3):
                    total = total + (term_in[k, d, 0].astype(F32) + term_in[k, d, 1].astype(F32))
                kept[k] = total

            for h in range(2):
                gb_all(it, h).wait_send()

        @stage(4)
        def _():
            it = i - 4
            fc_all(it).wait_recv()
            fd(it).start()
            fb_all(it).wait_send()

        @stage(3)
        def _():
            it = i - 3
            k = it % NS
            fb_all(it).wait_recv()
            s = (far[k, y].astype(F32) + far_y[k, 0].astype(F32)) + (
                far_y[k, 1].astype(F32) + far_y[k, 2].astype(F32)
            )
            full[k, 1, y, zh, :, rest] = s.astype(BF16)
            for d in range(3):
                fc(it, d).start()
            fa(it).wait_send()

        @stage(1)
        def _():
            it = i - 1
            v1_all(it).wait_recv()
            for h in range(2):
                project(it, 1 - h)
                if h == 0:
                    fa(it).start()
                for d in range(2):
                    ra(it, 1 - h, d).start()
            v0(it).wait_send()

        @stage(2)
        def _():
            it = i - 2
            k = it % NS
            fa(it).wait_recv()
            sums = part[k, 1, :, zh, :, rest].astype(F32) + far_in[k].astype(F32)
            far[k] = sums.astype(BF16)
            for d in range(3):
                fb(it, d).start()

        return 0

    lax.fori_loop(1, ITEMS + 8, run, 0)

    total = jnp.sum(squares[...].reshape(128, 128).T, axis=0, keepdims=True)
    sq[...] = jnp.broadcast_to(total, (8, 128))
    ys = [send(sq, sq_y.at[k], n_s.at[0], n_r.at[0], y_all[k]) for k in range(3)]
    for c in ys:
        c.start()

    def turn(side, r):
        cols = pl.ds(pl.multiple_of(side * HALF + r * 128, 128), 128)
        return upd[:, :, cols].reshape(128, 128).T

    for r in range(HALF // 128):
        turned[r * 128 : (r + 1) * 128, :] = turn(1 - core, r)
    swap = send(turned, turned_in, u_s.at[0], u_r.at[0], pair)
    swap.start()
    for r in range(HALF // 128):
        out_ref[r * 128 : (r + 1) * 128, pl.ds(pl.multiple_of(core * 128, 128), 128)] = turn(core, r)
    ys_all = send(sq_y, sq_y, n_s.at[0], n_r.at[0], zl_dev)
    ys_all.wait_recv()
    sq_sum[...] = (sq[...] + sq_y[0]) + (sq_y[1] + sq_y[2])
    ms = [
        send(sq_sum, sq_in.at[k], m_s.at[0], m_r.at[0], dev)
        for k, dev in enumerate((z_dev, pair, zc_dev))
    ]
    for c in ms:
        c.start()
    swap.wait_recv()
    out_ref[:, pl.ds(pl.multiple_of((1 - core) * 128, 128), 128)] = turned_in[...]
    ms_all = send(sq_in, sq_in, m_s.at[0], m_r.at[0], zl_dev)
    ms_all.wait_recv()
    own_norm = jnp.sqrt(sq_sum[0:1, :] + sq_in[0, 0:1, :])
    other_norm = jnp.sqrt(sq_in[1, 0:1, :] + sq_in[2, 0:1, :])
    norm_ref[0:1, :] = jnp.where(core == 0, own_norm, other_norm)
    norm_ref[1:2, :] = jnp.where(core == 0, other_norm, own_norm)
    for c in (*pairs, swap, ys_all, ms_all):
        c.wait_send()


def on_device(rotation, gradient):
    dma = pltpu.SemaphoreType.DMA

    def both(shape):
        return [dma(shape), dma(shape)]

    quarters = (4, 2, CH, BLK)
    updated, norms = pl.pallas_call(
        step_kernel,
        name="cayley_step",
        out_shape=(
            jax.ShapeDtypeStruct((HALF, 256), F32),
            jax.ShapeDtypeStruct((2, 128), F32),
        ),
        in_specs=[pl.BlockSpec(memory_space=pl.ANY)] * 2,
        out_specs=(
            pl.BlockSpec(memory_space=pltpu.VMEM),
            pl.BlockSpec(memory_space=pltpu.VMEM),
        ),
        scratch_shapes=[
            pltpu.VMEM((BLK, BLK), BF16),
            pltpu.VMEM((BLK, BLK), BF16),
            pltpu.VMEM((NS, CH, BLK), BF16),
            pltpu.VMEM((NS, CH, HALF), BF16),
            pltpu.VMEM((NS, *quarters), BF16),
            pltpu.VMEM((NS, 2, *quarters), BF16),
            pltpu.VMEM((NS, 2, *quarters), BF16),
            pltpu.VMEM((NS, 2, 2, CH, BLK), BF16),
            pltpu.VMEM((NS, 2, 2, CH, BLK), BF16),
            pltpu.VMEM((NS, 2, 2, 2, CH, BLK), BF16),
            pltpu.VMEM((NS, 2, 2, CH, BLK), BF16),
            pltpu.VMEM((NS, 4, CH, BLK - CUT), BF16),
            pltpu.VMEM((NS, 4, CH, BLK - CUT), BF16),
            pltpu.VMEM((NS, 3, CH, BLK - CUT), BF16),
            pltpu.VMEM((NS, *quarters), BF16),
            pltpu.VMEM((NS, 3, 2, CH, BLK), BF16),
            pltpu.VMEM((NS, CH, BLK), F32),
            pltpu.VMEM((NS, CH, BLK), BF16),
            pltpu.VMEM((NS, CH, BLK), BF16),
            pltpu.VMEM((NS, CH, BLK), F32),
            pltpu.VMEM((NS, CH, 128), F32),
            pltpu.VMEM((HALF, 128), F32),
            pltpu.VMEM((HALF, 128), F32),
            pltpu.VMEM((8, 128), F32),
            pltpu.VMEM((3, 8, 128), F32),
            pltpu.VMEM((8, 128), F32),
            pltpu.VMEM((3, 8, 128), F32),
            dma((2,)),
            *both((3,)),
            *both((NS,)),
            *both((NS,)),
            *both((NQ, 2)),
            *both((NQ, 2)),
            *both((NQ, 2)),
            *both((NL, 2)),
            *both((NL, 2)),
            *both((NL,)),
            *both((NQ,)),
            *both((NQ,)),
            *both((NL,)),
            *both((NL,)),
            *both((NL,)),
            *both((1,)),
            *both((1,)),
            *both((1,)),
        ],
        compiler_params=pltpu.CompilerParams(
            collective_id=1, has_side_effects=True, vmem_limit_bytes=62 * 1024 * 1024
        ),
        cost_estimate=pl.CostEstimate(
            flops=20_000_000_000, bytes_accessed=3_000_000, transcendentals=0
        ),
    )(rotation, gradient)
    return updated, norms.reshape(256)


def solution(mesh):
    placed = (P("row", "col"), P("row", "col"))
    return jax.shard_map(
        on_device,
        mesh=mesh,
        in_specs=placed,
        out_specs=(P("row", "col"), P("col")),
        check_vma=False,
    )
```

```python
import jax
import jax.numpy as jnp
from jax import lax
from jax.experimental import pallas as pl
from jax.experimental.pallas import tpu as pltpu
from jax.sharding import PartitionSpec as P

MESH = pl.DeviceIdType.MESH
F32 = jnp.float32
BF16 = jnp.bfloat16
NS = 8
CH = 16
BLK = 1024
HALF = 512
TILE = 512
ITEMS = 2 * NS
NQ = 2
NL = 4
CUT = 384
WIDE = (BLK, CUT)
LATE = ITEMS - 1


def step_kernel(
    rot_hbm, grad_hbm, out_ref, norm_ref,
    rot, grad, base, base_out, panel, part, full, mine, ring_a, ring_b, swapped, far, far_in, far_y,
    term, term_in, kept, tail, tail_in, upd, squares, turned, turned_in, sq, sq_in,
    load_sem, pair_s, pair_r, v0_s, v0_r, v1_s, v1_r, a_s, a_r, b_s, b_r, z_s, z_r,
    c_s, c_r, e_s, e_r, fa_s, fa_r, fb_s, fb_r, fc_s, fc_r, fd_s, fd_r, t_s, t_r, w_s, w_r, u_s, u_r, n_s, n_r,
):
    row = lax.axis_index("row")
    col = lax.axis_index("col")
    core, y, zh = row % 2, (row // 2) % 4, row // 8
    x, zl = col // 2, col % 2
    up, across, down = (y + 1) % 4, (y + 2) % 4, (y + 3) % 4

    def at_row(zh_, y_, core_):
        return {"row": zh_ * 8 + y_ * 2 + core_, "col": col}

    def at_col(x_, zl_):
        return {"row": row, "col": x_ * 2 + zl_}

    pair = at_row(zh, y, 1 - core)
    y_dev = (at_row(zh, up, core), at_row(zh, down, core))
    y_q = (up, down)
    y_all = tuple(at_row(zh, (y + k) % 4, core) for k in (1, 2, 3))
    z_dev = at_row(1 - zh, y, core)
    x_all = tuple(at_col((x + k) % 4, zl) for k in (1, 2, 3))
    x_far = tuple(at_col((x + k) % 4, 1 - zl) for k in (1, 2, 3))
    zl_dev = at_col(x, 1 - zl)

    def send(src, dst, s, r, dev):
        return pltpu.make_async_remote_copy(
            src_ref=src, dst_ref=dst, send_sem=s, recv_sem=r, device_id=dev, device_id_type=MESH
        )

    own_rows = pl.ds(pl.multiple_of(core * HALF, HALF), HALF)
    other_rows = pl.ds(pl.multiple_of((1 - core) * HALF, HALF), HALF)
    loads = [
        pltpu.make_async_copy(rot_hbm, rot.at[own_rows], load_sem.at[0]),
        pltpu.make_async_copy(grad_hbm, grad.at[own_rows], load_sem.at[1]),
    ]
    for c in loads:
        c.start()

    barrier = pltpu.get_barrier_semaphore()
    peers = (pair, *y_dev, z_dev, *x_all, zl_dev)
    for dev in peers:
        pl.semaphore_signal(barrier, inc=1, device_id=dev, device_id_type=MESH)

    pick = lax.broadcasted_iota(jnp.int32, (128, HALF), 1) == 4 * lax.broadcasted_iota(
        jnp.int32, (128, HALF), 0
    )
    pick = pick.astype(F32).astype(BF16)

    def picked(side):
        cols = pl.ds(pl.multiple_of(side * HALF, HALF), HALF)
        return (
            lax.dot_general(
                pick, rot[own_rows, cols], (((1,), (1,)), ((), ())), preferred_element_type=F32
            )
            .astype(BF16)
            .reshape(NS, CH, HALF)
        )

    loads[0].wait()
    base_out[...] = picked(1 - core)
    base[:, :, own_rows] = picked(core)
    loads[1].wait()

    pl.semaphore_wait(barrier, len(peers))
    pairs = [
        send(base_out, base.at[:, :, own_rows], pair_s.at[0], pair_r.at[0], pair),
        send(rot.at[own_rows], rot.at[own_rows], pair_s.at[1], pair_r.at[1], pair),
        send(grad.at[own_rows], grad.at[own_rows], pair_s.at[2], pair_r.at[2], pair),
    ]
    for c in pairs:
        c.start()
    pairs[0].wait_recv()

    def first(h):
        return pl.ds(0, WIDE[h])

    rest = pl.ds(CUT, BLK - CUT)

    def v0(i):
        k = i % NS
        return send(panel.at[k, x, zl], panel.at[k, x, zl], v0_s.at[k], v0_r.at[k], zl_dev)

    def v1(i, d):
        k = i % NS
        return send(panel.at[k, x], panel.at[k, x], v1_s.at[k], v1_r.at[k], x_all[d])

    def v1_all(i):
        k = i % NS
        return send(term_in.at[k], term_in.at[k], v1_s.at[k], v1_r.at[k], zl_dev)

    def ra(i, h, d):
        k, q = i % NS, i % NQ
        return send(
            part.at[k, h, across, d, :, first(h)],
            ring_a.at[k, h, d, :, first(h)],
            a_s.at[q, h],
            a_r.at[q, h],
            y_dev[d],
        )

    def ra_all(i, h):
        k, q = i % NS, i % NQ
        ref = ring_a.at[k, h, :, :, first(h)]
        return send(ref, ref, a_s.at[q, h], a_r.at[q, h], zl_dev)

    def rb(i, h, d):
        k, q = i % NS, i % NQ
        return send(
            part.at[k, h, y_q[d], :, :, first(h)],
            ring_b.at[k, h, d, :, :, first(h)],
            b_s.at[q, h],
            b_r.at[q, h],
            y_dev[d],
        )

    def rb_all(i, h):
        k, q = i % NS, i % NQ
        ref = ring_b.at[k, h, :, :, :, first(h)]
        return send(ref, ref, b_s.at[q, h], b_r.at[q, h], zl_dev)

    def zx(i, h):
        k, q = i % NS, i % NQ
        return send(
            mine.at[k, h, :, :, first(h)],
            swapped.at[k, h, :, :, first(h)],
            z_s.at[q, h],
            z_r.at[q, h],
            z_dev,
        )

    def ga(i, h, d):
        k, q = i % NS, i % NL
        place = full.at[k, h, y, :, :, first(h)]
        return send(place, place, c_s.at[q, h], c_r.at[q, h], y_dev[d])

    def ga_all(i, h):
        k, q = i % NS, i % NL
        ref = ring_b.at[k, h, :, :, :, first(h)]
        return send(ref, ref, c_s.at[q, h], c_r.at[q, h], zl_dev)

    def gb(i, h, d):
        k, q = i % NS, i % NL
        place = full.at[k, h, y_q[1 - d], d, :, first(h)]
        return send(place, place, e_s.at[q, h], e_r.at[q, h], y_dev[d])

    def gb_all(i, h):
        k, q = i % NS, i % NL
        ref = ring_a.at[k, h, :, :, first(h)]
        return send(ref, ref, e_s.at[q, h], e_r.at[q, h], zl_dev)

    def fa(i):
        k, q = i % NS, i % NL
        return send(
            part.at[k, 1, :, 1 - zh, :, rest], far_in.at[k], fa_s.at[q], fa_r.at[q], z_dev
        )

    def fb(i, d):
        k, q = i % NS, i % NQ
        return send(
            far.at[k, (y + d + 1) % 4], far_y.at[k, d], fb_s.at[q], fb_r.at[q], y_all[d]
        )

    def fb_all(i):
        k, q = i % NS, i % NQ
        return send(far_y.at[k], far_y.at[k], fb_s.at[q], fb_r.at[q], zl_dev)

    def fc(i, d):
        k, q = i % NS, i % NQ
        place = full.at[k, 1, y, zh, :, rest]
        return send(place, place, fc_s.at[q], fc_r.at[q], y_all[d])

    def fc_all(i):
        k, q = i % NS, i % NQ
        return send(far_y.at[k], far_y.at[k], fc_s.at[q], fc_r.at[q], zl_dev)

    def fd(i):
        k, q = i % NS, i % NL
        place = full.at[k, 1, :, zh, :, rest]
        return send(place, place, fd_s.at[q], fd_r.at[q], z_dev)

    def tx(i, d):
        k, q = i % NS, i % NL
        return send(
            term.at[k, (x + d + 1) % 4], term_in.at[k, d], t_s.at[q], t_r.at[q], x_all[d]
        )

    def tx_all(i):
        k, q = i % NS, i % NL
        return send(term_in.at[k], term_in.at[k], t_s.at[q], t_r.at[q], zl_dev)

    def wz(i):
        k, q = i % NS, i % NL
        return send(tail.at[k], tail_in.at[k], w_s.at[q], w_r.at[q], zl_dev)

    for j in range(NS):
        panel[j, x, zl] = base[j]
    for j in range(NS):
        v0(j).start()
    for j in range(NS):
        v0(j).wait_recv()
        for d in range(3):
            v1(j, d).start()
    pairs[1].wait_recv()
    pairs[2].wait_recv()

    def project(i, h):
        k = i % NS
        held = (rot, grad)[h]
        lhs = panel[k].reshape(8 * CH, BLK)

        @pl.loop(0, BLK // TILE)
        def _(n):
            cols = pl.ds(pl.multiple_of(n * TILE, TILE), TILE)
            z = jnp.dot(lhs, held[:, cols], preferred_element_type=F32)
            part[k, h, :, :, :, cols] = z.astype(BF16).reshape(4, 2, CH, TILE)

    def apply(i):
        k = i % NS

        @pl.loop(0, BLK // TILE)
        def _(n):
            rows = pl.ds(pl.multiple_of(n * TILE, TILE), TILE)
            nt = (((1,), (1,)), ((), ()))
            t = lax.dot_general(
                full[k, 0].reshape(8 * CH, BLK), grad[rows, :], nt, preferred_element_type=F32
            ) - lax.dot_general(
                full[k, 1].reshape(8 * CH, BLK), rot[rows, :], nt, preferred_element_type=F32
            )
            term[k, :, :, :, rows] = t.astype(BF16).reshape(4, 2, CH, TILE)

    def run(i, _):
        def stage(late):
            return pl.when((i >= late) & (i < ITEMS + late))

        @pl.when((i > NS) & (i <= ITEMS))
        def _():
            v0(i - 1).wait_recv()
            for d in range(3):
                v1(i - 1, d).start()

        @stage(5)
        def _():
            it = i - 5
            for h in range(2):
                ga_all(it, h).wait_recv()
                for d in range(2):
                    gb(it, h, d).start()
            for h in range(2):
                zx(it, h).wait_send()
            fc_all(it).wait_send()

        @stage(4)
        def _():
            it = i - 4
            k = it % NS
            for h in range(2):
                zx(it, h).wait_recv()
                w = first(h)
                z = mine[k, h, :, :, w].astype(F32) + swapped[k, h, :, :, w].astype(F32)
                full[k, h, y, :, :, w] = z.astype(BF16)
                for d in range(2):
                    ga(it, h, d).start()
            for h in range(2):
                rb_all(it, h).wait_send()

        @stage(3)
        def _():
            it = i - 3
            k = it % NS
            for h in range(2):
                rb_all(it, h).wait_recv()
                w = first(h)
                s = part[k, h, y, :, :, w].astype(F32) + (
                    ring_b[k, h, 0, :, :, w].astype(F32) + ring_b[k, h, 1, :, :, w].astype(F32)
                )
                mine[k, h, :, :, w] = s.astype(BF16)
                zx(it, h).start()
            for h in range(2):
                ra_all(it, h).wait_send()

        @stage(8)
        def _():
            it = i - 8
            k = it % NS
            wz(it).wait_recv()
            applied = kept[k] + tail_in[k].astype(F32)
            b = base[k].astype(F32)

            @pl.when(i < ITEMS)
            def _():
                first = b + 0.25 * applied
                panel[k, x, zl] = (b + first).astype(BF16)
                v0(i).start()

            @pl.when(i >= ITEMS)
            def _():
                new = b + 0.125 * applied
                upd[k] = new
                lanes = new[:, :128] * new[:, :128]
                for r in range(1, BLK // 128):
                    lane = new[:, r * 128 : (r + 1) * 128]
                    lanes = lanes + lane * lane
                squares[k] = lanes

            tx_all(it).wait_send()
            wz(it).wait_send()

        @stage(2)
        def _():
            it = i - 2
            k = it % NS
            for h in range(2):
                w = first(h)
                ra_all(it, h).wait_recv()
                for d in range(2):
                    there = part[k, h, y_q[d], d, :, w].astype(F32)
                    there = there + ring_a[k, h, d, :, w].astype(F32)
                    part[k, h, y_q[d], d, :, w] = there.astype(BF16)
                    rb(it, h, d).start()
            v1_all(it).wait_send()

        @stage(6)
        def _():
            it = i - 6
            for h in range(2):
                gb_all(it, h).wait_recv()
            fd(it).wait_recv()
            apply(it)
            k, q = it % NS, it % NL

            @pl.when(it < LATE)
            def _():
                for d in range(3):
                    tx(it, d).start()

            @pl.when(it >= LATE)
            def _():
                for d in range(3):
                    for z, dev in ((0, x_all[d]), (1, x_far[d])):
                        src = term.at[k, (x + d + 1) % 4, zl + z - 2 * zl * z]
                        send(src, term_in.at[k, d, z], t_s.at[q], t_r.at[q], dev).start()
                send(term.at[k, x, 1 - zl], tail_in.at[k], w_s.at[q], w_r.at[q], zl_dev).start()

            for h in range(2):
                ga_all(it, h).wait_send()
            fd(it).wait_send()

        @stage(7)
        def _():
            it = i - 7
            k = it % NS
            tx_all(it).wait_recv()

            def summed(z):
                return (term[k, x, z].astype(F32) + term_in[k, 0, z].astype(F32)) + (
                    term_in[k, 1, z].astype(F32) + term_in[k, 2, z].astype(F32)
                )

            @pl.when(it < LATE)
            def _():
                tail[k] = summed(1 - zl).astype(BF16)
                wz(it).start()
                kept[k] = summed(zl)

            @pl.when(it >= LATE)
            def _():
                total = term[k, x, zl].astype(F32)
                for d in range(3):
                    total = total + (term_in[k, d, 0].astype(F32) + term_in[k, d, 1].astype(F32))
                kept[k] = total

            for h in range(2):
                gb_all(it, h).wait_send()

        @stage(4)
        def _():
            it = i - 4
            fc_all(it).wait_recv()
            fd(it).start()
            fb_all(it).wait_send()

        @stage(3)
        def _():
            it = i - 3
            k = it % NS
            fb_all(it).wait_recv()
            s = (far[k, y].astype(F32) + far_y[k, 0].astype(F32)) + (
                far_y[k, 1].astype(F32) + far_y[k, 2].astype(F32)
            )
            full[k, 1, y, zh, :, rest] = s.astype(BF16)
            for d in range(3):
                fc(it, d).start()
            fa(it).wait_send()

        @stage(1)
        def _():
            it = i - 1
            v1_all(it).wait_recv()
            for h in range(2):
                project(it, 1 - h)
                if h == 0:
                    fa(it).start()
                for d in range(2):
                    ra(it, 1 - h, d).start()
            v0(it).wait_send()

        @stage(2)
        def _():
            it = i - 2
            k = it % NS
            fa(it).wait_recv()
            sums = part[k, 1, :, zh, :, rest].astype(F32) + far_in[k].astype(F32)
            far[k] = sums.astype(BF16)
            for d in range(3):
                fb(it, d).start()

        return 0

    lax.fori_loop(1, ITEMS + 8, run, 0)

    total = jnp.sum(squares[...].reshape(128, 128).T, axis=0, keepdims=True)
    sq[...] = jnp.broadcast_to(total, (8, 128))
    sums = []
    for z in range(2):
        for k in range(4):
            for c in range(2):
                if (z, k, c) != (0, 0, 0):
                    dev = at_row((zh + z) % 2, (y + k) % 4, (core + c) % 2)
                    sums.append(send(sq, sq_in.at[row], n_s.at[0], n_r.at[0], dev))
    for c in sums:
        c.start()
    sq_in[row] = sq[...]

    def turn(side, r):
        cols = pl.ds(pl.multiple_of(side * HALF + r * 128, 128), 128)
        return upd[:, :, cols].reshape(128, 128).T

    for r in range(HALF // 128):
        turned[r * 128 : (r + 1) * 128, :] = turn(1 - core, r)
    swap = send(turned, turned_in, u_s.at[0], u_r.at[0], pair)
    swap.start()
    for r in range(HALF // 128):
        out_ref[r * 128 : (r + 1) * 128, pl.ds(pl.multiple_of(core * 128, 128), 128)] = turn(core, r)
    swap.wait_recv()
    out_ref[:, pl.ds(pl.multiple_of((1 - core) * 128, 128), 128)] = turned_in[...]
    others = sq_in.at[pl.ds(0, 15)]
    sums_all = send(others, others, n_s.at[0], n_r.at[0], zl_dev)
    sums_all.wait_recv()
    for c in range(2):
        total = sq_in[c, 0:1, :]
        for r in range(c + 2, 16, 2):
            total = total + sq_in[r, 0:1, :]
        norm_ref[c : c + 1, :] = jnp.sqrt(total)
    for c in (*pairs, swap, sums_all):
        c.wait_send()


def on_device(rotation, gradient):
    dma = pltpu.SemaphoreType.DMA

    def both(shape):
        return [dma(shape), dma(shape)]

    quarters = (4, 2, CH, BLK)
    updated, norms = pl.pallas_call(
        step_kernel,
        name="cayley_step",
        out_shape=(
            jax.ShapeDtypeStruct((HALF, 256), F32),
            jax.ShapeDtypeStruct((2, 128), F32),
        ),
        in_specs=[pl.BlockSpec(memory_space=pl.ANY)] * 2,
        out_specs=(
            pl.BlockSpec(memory_space=pltpu.VMEM),
            pl.BlockSpec(memory_space=pltpu.VMEM),
        ),
        scratch_shapes=[
            pltpu.VMEM((BLK, BLK), BF16),
            pltpu.VMEM((BLK, BLK), BF16),
            pltpu.VMEM((NS, CH, BLK), BF16),
            pltpu.VMEM((NS, CH, HALF), BF16),
            pltpu.VMEM((NS, *quarters), BF16),
            pltpu.VMEM((NS, 2, *quarters), BF16),
            pltpu.VMEM((NS, 2, *quarters), BF16),
            pltpu.VMEM((NS, 2, 2, CH, BLK), BF16),
            pltpu.VMEM((NS, 2, 2, CH, BLK), BF16),
            pltpu.VMEM((NS, 2, 2, 2, CH, BLK), BF16),
            pltpu.VMEM((NS, 2, 2, CH, BLK), BF16),
            pltpu.VMEM((NS, 4, CH, BLK - CUT), BF16),
            pltpu.VMEM((NS, 4, CH, BLK - CUT), BF16),
            pltpu.VMEM((NS, 3, CH, BLK - CUT), BF16),
            pltpu.VMEM((NS, *quarters), BF16),
            pltpu.VMEM((NS, 3, 2, CH, BLK), BF16),
            pltpu.VMEM((NS, CH, BLK), F32),
            pltpu.VMEM((NS, CH, BLK), BF16),
            pltpu.VMEM((NS, CH, BLK), BF16),
            pltpu.VMEM((NS, CH, BLK), F32),
            pltpu.VMEM((NS, CH, 128), F32),
            pltpu.VMEM((HALF, 128), F32),
            pltpu.VMEM((HALF, 128), F32),
            pltpu.VMEM((8, 128), F32),
            pltpu.VMEM((16, 8, 128), F32),
            dma((2,)),
            *both((3,)),
            *both((NS,)),
            *both((NS,)),
            *both((NQ, 2)),
            *both((NQ, 2)),
            *both((NQ, 2)),
            *both((NL, 2)),
            *both((NL, 2)),
            *both((NL,)),
            *both((NQ,)),
            *both((NQ,)),
            *both((NL,)),
            *both((NL,)),
            *both((NL,)),
            *both((1,)),
            *both((1,)),
        ],
        compiler_params=pltpu.CompilerParams(
            collective_id=1, has_side_effects=True, vmem_limit_bytes=53 * 1024 * 1024
        ),
        cost_estimate=pl.CostEstimate(
            flops=20_000_000_000, bytes_accessed=3_000_000, transcendentals=0
        ),
    )(rotation, gradient)
    return updated, norms.reshape(256)


def solution(mesh):
    placed = (P("row", "col"), P("row", "col"))
    return jax.shard_map(
        on_device,
        mesh=mesh,
        in_specs=placed,
        out_specs=(P("row", "col"), P("col")),
        check_vma=False,
    )
```

```python
import jax
import jax.numpy as jnp
from jax import lax
from jax.experimental import pallas as pl
from jax.experimental.pallas import tpu as pltpu
from jax.sharding import PartitionSpec as P

MESH = pl.DeviceIdType.MESH
F32 = jnp.float32
BF16 = jnp.bfloat16
NS = 8
CH = 16
BLK = 1024
HALF = 512
TILE = 1024
ITEMS = 2 * NS
NQ = 2
NL = 4
CUT = 256
WIDE = (BLK, CUT)
LATE = ITEMS - 1


def step_kernel(
    rot_hbm, grad_hbm, out_ref, norm_ref,
    rot, grad, base, base_out, panel, part, full, mine, ring_a, ring_b, swapped, far, far_in, far_y,
    term, term_in, kept, tail, tail_in, upd, squares, turned, turned_in, sq, sq_in,
    load_sem, pair_s, pair_r, v0_s, v0_r, v1_s, v1_r, a_s, a_r, b_s, b_r, z_s, z_r,
    c_s, c_r, e_s, e_r, fa_s, fa_r, fb_s, fb_r, fc_s, fc_r, fd_s, fd_r, t_s, t_r, w_s, w_r, u_s, u_r, n_s, n_r,
):
    row = lax.axis_index("row")
    col = lax.axis_index("col")
    core, y, zh = row % 2, (row // 2) % 4, row // 8
    x, zl = col // 2, col % 2
    up, across, down = (y + 1) % 4, (y + 2) % 4, (y + 3) % 4

    def at_row(zh_, y_, core_):
        return {"row": zh_ * 8 + y_ * 2 + core_, "col": col}

    def at_col(x_, zl_):
        return {"row": row, "col": x_ * 2 + zl_}

    pair = at_row(zh, y, 1 - core)
    y_dev = (at_row(zh, up, core), at_row(zh, down, core))
    y_q = (up, down)
    y_all = tuple(at_row(zh, (y + k) % 4, core) for k in (1, 2, 3))
    z_dev = at_row(1 - zh, y, core)
    x_all = tuple(at_col((x + k) % 4, zl) for k in (1, 2, 3))
    x_far = tuple(at_col((x + k) % 4, 1 - zl) for k in (1, 2, 3))
    zl_dev = at_col(x, 1 - zl)
    zl_pair = {"row": zh * 8 + y * 2 + 1 - core, "col": x * 2 + 1 - zl}

    def send(src, dst, s, r, dev):
        return pltpu.make_async_remote_copy(
            src_ref=src, dst_ref=dst, send_sem=s, recv_sem=r, device_id=dev, device_id_type=MESH
        )

    own_rows = pl.ds(pl.multiple_of(core * HALF, HALF), HALF)
    other_rows = pl.ds(pl.multiple_of((1 - core) * HALF, HALF), HALF)
    loads = [
        pltpu.make_async_copy(rot_hbm, rot.at[own_rows], load_sem.at[0]),
        pltpu.make_async_copy(grad_hbm, grad.at[own_rows], load_sem.at[1]),
    ]
    for c in loads:
        c.start()

    barrier = pltpu.get_barrier_semaphore()
    peers = (pair, *y_dev, z_dev, *x_all, zl_dev, zl_pair)
    for dev in peers:
        pl.semaphore_signal(barrier, inc=1, device_id=dev, device_id_type=MESH)

    pick = lax.broadcasted_iota(jnp.int32, (128, HALF), 1) == 4 * lax.broadcasted_iota(
        jnp.int32, (128, HALF), 0
    )
    pick = pick.astype(F32).astype(BF16)

    def picked(side):
        cols = pl.ds(pl.multiple_of(side * HALF, HALF), HALF)
        return (
            lax.dot_general(
                pick, rot[own_rows, cols], (((1,), (1,)), ((), ())), preferred_element_type=F32
            )
            .astype(BF16)
            .reshape(NS, CH, HALF)
        )

    loads[0].wait()
    base_out[...] = picked(1 - core)
    base[:, :, own_rows] = picked(core)
    panel[0, x, zl, :, own_rows] = base[0, :, own_rows]
    loads[1].wait()

    pl.semaphore_wait(barrier, len(peers))
    pairs = [
        send(base_out, base.at[:, :, own_rows], pair_s.at[0], pair_r.at[0], pair),
        send(rot.at[own_rows], rot.at[own_rows], pair_s.at[1], pair_r.at[1], pair),
        send(grad.at[own_rows], grad.at[own_rows], pair_s.at[2], pair_r.at[2], pair),
    ]
    pairs[0].start()
    there = panel.at[0, x, zl, :, own_rows]
    send(there, there, v0_s.at[0], v0_r.at[0], zl_dev).start()
    send(base_out.at[0], there, v0_s.at[0], v0_r.at[0], zl_pair).start()
    for c in pairs[1:]:
        c.start()
    pairs[0].wait_recv()

    def first(h):
        return pl.ds(0, WIDE[h])

    rest = pl.ds(CUT, BLK - CUT)

    def v0(i):
        k = i % NS
        return send(panel.at[k, x, zl], panel.at[k, x, zl], v0_s.at[k], v0_r.at[k], zl_dev)

    def v1(i, d):
        k = i % NS
        return send(panel.at[k, x], panel.at[k, x], v1_s.at[k], v1_r.at[k], x_all[d])

    def v1_all(i):
        k = i % NS
        return send(term_in.at[k], term_in.at[k], v1_s.at[k], v1_r.at[k], zl_dev)

    def ra(i, h, d):
        k, q = i % NS, i % NQ
        return send(
            part.at[k, h, across, d, :, first(h)],
            ring_a.at[k, h, d, :, first(h)],
            a_s.at[q, h],
            a_r.at[q, h],
            y_dev[d],
        )

    def ra_all(i, h):
        k, q = i % NS, i % NQ
        ref = ring_a.at[k, h, :, :, first(h)]
        return send(ref, ref, a_s.at[q, h], a_r.at[q, h], zl_dev)

    def rb(i, h, d):
        k, q = i % NS, i % NQ
        return send(
            part.at[k, h, y_q[d], :, :, first(h)],
            ring_b.at[k, h, d, :, :, first(h)],
            b_s.at[q, h],
            b_r.at[q, h],
            y_dev[d],
        )

    def rb_all(i, h):
        k, q = i % NS, i % NQ
        ref = ring_b.at[k, h, :, :, :, first(h)]
        return send(ref, ref, b_s.at[q, h], b_r.at[q, h], zl_dev)

    def zx(i, h):
        k, q = i % NS, i % NQ
        return send(
            mine.at[k, h, :, :, first(h)],
            swapped.at[k, h, :, :, first(h)],
            z_s.at[q, h],
            z_r.at[q, h],
            z_dev,
        )

    def ga(i, h, d):
        k, q = i % NS, i % NL
        place = full.at[k, h, y, :, :, first(h)]
        return send(place, place, c_s.at[q, h], c_r.at[q, h], y_dev[d])

    def ga_all(i, h):
        k, q = i % NS, i % NL
        ref = ring_b.at[k, h, :, :, :, first(h)]
        return send(ref, ref, c_s.at[q, h], c_r.at[q, h], zl_dev)

    def gb(i, h, d):
        k, q = i % NS, i % NL
        place = full.at[k, h, y_q[1 - d], d, :, first(h)]
        return send(place, place, e_s.at[q, h], e_r.at[q, h], y_dev[d])

    def gb_all(i, h):
        k, q = i % NS, i % NL
        ref = ring_a.at[k, h, :, :, first(h)]
        return send(ref, ref, e_s.at[q, h], e_r.at[q, h], zl_dev)

    def fa(i):
        k, q = i % NS, i % NL
        return send(
            part.at[k, 1, :, 1 - zh, :, rest], far_in.at[k], fa_s.at[q], fa_r.at[q], z_dev
        )

    def fb(i, d):
        k, q = i % NS, i % NQ
        return send(
            far.at[k, (y + d + 1) % 4], far_y.at[k, d], fb_s.at[q], fb_r.at[q], y_all[d]
        )

    def fb_all(i):
        k, q = i % NS, i % NQ
        return send(far_y.at[k], far_y.at[k], fb_s.at[q], fb_r.at[q], zl_dev)

    def fc(i, d):
        k, q = i % NS, i % NQ
        place = full.at[k, 1, y, zh, :, rest]
        return send(place, place, fc_s.at[q], fc_r.at[q], y_all[d])

    def fc_all(i):
        k, q = i % NS, i % NQ
        return send(far_y.at[k], far_y.at[k], fc_s.at[q], fc_r.at[q], zl_dev)

    def fd(i):
        k, q = i % NS, i % NL
        place = full.at[k, 1, :, zh, :, rest]
        return send(place, place, fd_s.at[q], fd_r.at[q], z_dev)

    def tx(i, d):
        k, q = i % NS, i % NL
        return send(
            term.at[k, (x + d + 1) % 4], term_in.at[k, d], t_s.at[q], t_r.at[q], x_all[d]
        )

    def tx_all(i):
        k, q = i % NS, i % NL
        return send(term_in.at[k], term_in.at[k], t_s.at[q], t_r.at[q], zl_dev)

    def wz(i):
        k, q = i % NS, i % NL
        return send(tail.at[k], tail_in.at[k], w_s.at[q], w_r.at[q], zl_dev)

    panel[0, x, zl, :, other_rows] = base[0, :, other_rows]
    for j in range(1, NS):
        panel[j, x, zl] = base[j]
    for j in range(1, NS):
        v0(j).start()
    for j in range(NS):
        v0(j).wait_recv()
        for d in range(3):
            v1(j, d).start()
    pairs[1].wait_recv()
    pairs[2].wait_recv()

    def project(i, h):
        k = i % NS
        held = (rot, grad)[h]
        lhs = panel[k].reshape(8 * CH, BLK)

        @pl.loop(0, BLK // TILE)
        def _(n):
            cols = pl.ds(pl.multiple_of(n * TILE, TILE), TILE)
            z = jnp.dot(lhs, held[:, cols], preferred_element_type=F32)
            part[k, h, :, :, :, cols] = z.astype(BF16).reshape(4, 2, CH, TILE)

    def apply(i):
        k = i % NS

        @pl.loop(0, BLK // TILE)
        def _(n):
            rows = pl.ds(pl.multiple_of(n * TILE, TILE), TILE)
            nt = (((1,), (1,)), ((), ()))
            t = lax.dot_general(
                full[k, 0].reshape(8 * CH, BLK), grad[rows, :], nt, preferred_element_type=F32
            ) - lax.dot_general(
                full[k, 1].reshape(8 * CH, BLK), rot[rows, :], nt, preferred_element_type=F32
            )
            term[k, :, :, :, rows] = t.astype(BF16).reshape(4, 2, CH, TILE)

    def run(i, _):
        def stage(late):
            return pl.when((i >= late) & (i < ITEMS + late))

        @pl.when((i > NS) & (i <= ITEMS))
        def _():
            v0(i - 1).wait_recv()
            for d in range(3):
                v1(i - 1, d).start()

        @stage(5)
        def _():
            it = i - 5
            for h in range(2):
                ga_all(it, h).wait_recv()
                for d in range(2):
                    gb(it, h, d).start()
            for h in range(2):
                zx(it, h).wait_send()
            fc_all(it).wait_send()

        @stage(4)
        def _():
            it = i - 4
            k = it % NS
            for h in range(2):
                zx(it, h).wait_recv()
                w = first(h)
                z = mine[k, h, :, :, w].astype(F32) + swapped[k, h, :, :, w].astype(F32)
                full[k, h, y, :, :, w] = z.astype(BF16)
                for d in range(2):
                    ga(it, h, d).start()
            for h in range(2):
                rb_all(it, h).wait_send()

        @stage(3)
        def _():
            it = i - 3
            k = it % NS
            for h in range(2):
                rb_all(it, h).wait_recv()
                w = first(h)
                s = part[k, h, y, :, :, w].astype(F32) + (
                    ring_b[k, h, 0, :, :, w].astype(F32) + ring_b[k, h, 1, :, :, w].astype(F32)
                )
                mine[k, h, :, :, w] = s.astype(BF16)
                zx(it, h).start()
            for h in range(2):
                ra_all(it, h).wait_send()

        @stage(8)
        def _():
            it = i - 8
            k = it % NS
            wz(it).wait_recv()
            applied = kept[k] + tail_in[k].astype(F32)
            b = base[k].astype(F32)

            @pl.when(i < ITEMS)
            def _():
                first = b + 0.25 * applied
                panel[k, x, zl] = (b + first).astype(BF16)
                v0(i).start()

            @pl.when(i >= ITEMS)
            def _():
                new = b + 0.125 * applied
                upd[k] = new
                lanes = new[:, :128] * new[:, :128]
                for r in range(1, BLK // 128):
                    lane = new[:, r * 128 : (r + 1) * 128]
                    lanes = lanes + lane * lane
                squares[k] = lanes

            tx_all(it).wait_send()
            wz(it).wait_send()

        @stage(2)
        def _():
            it = i - 2
            k = it % NS
            for h in range(2):
                w = first(h)
                ra_all(it, h).wait_recv()
                for d in range(2):
                    there = part[k, h, y_q[d], d, :, w].astype(F32)
                    there = there + ring_a[k, h, d, :, w].astype(F32)
                    part[k, h, y_q[d], d, :, w] = there.astype(BF16)
                    rb(it, h, d).start()
            v1_all(it).wait_send()

        @stage(6)
        def _():
            it = i - 6
            for h in range(2):
                gb_all(it, h).wait_recv()
            fd(it).wait_recv()
            apply(it)
            k, q = it % NS, it % NL

            @pl.when(it < LATE)
            def _():
                for d in range(3):
                    tx(it, d).start()

            @pl.when(it >= LATE)
            def _():
                for d in range(3):
                    for z, dev in ((0, x_all[d]), (1, x_far[d])):
                        src = term.at[k, (x + d + 1) % 4, zl + z - 2 * zl * z]
                        send(src, term_in.at[k, d, z], t_s.at[q], t_r.at[q], dev).start()
                send(term.at[k, x, 1 - zl], tail_in.at[k], w_s.at[q], w_r.at[q], zl_dev).start()

            for h in range(2):
                ga_all(it, h).wait_send()
            fd(it).wait_send()

        @stage(7)
        def _():
            it = i - 7
            k = it % NS
            tx_all(it).wait_recv()

            def summed(z):
                return (term[k, x, z].astype(F32) + term_in[k, 0, z].astype(F32)) + (
                    term_in[k, 1, z].astype(F32) + term_in[k, 2, z].astype(F32)
                )

            @pl.when(it < LATE)
            def _():
                tail[k] = summed(1 - zl).astype(BF16)
                wz(it).start()
                kept[k] = summed(zl)

            @pl.when(it >= LATE)
            def _():
                total = term[k, x, zl].astype(F32)
                for d in range(3):
                    total = total + (term_in[k, d, 0].astype(F32) + term_in[k, d, 1].astype(F32))
                kept[k] = total

            for h in range(2):
                gb_all(it, h).wait_send()

        @stage(4)
        def _():
            it = i - 4
            fc_all(it).wait_recv()
            fd(it).start()
            fb_all(it).wait_send()

        @stage(3)
        def _():
            it = i - 3
            k = it % NS
            fb_all(it).wait_recv()
            s = (far[k, y].astype(F32) + far_y[k, 0].astype(F32)) + (
                far_y[k, 1].astype(F32) + far_y[k, 2].astype(F32)
            )
            full[k, 1, y, zh, :, rest] = s.astype(BF16)
            for d in range(3):
                fc(it, d).start()
            fa(it).wait_send()

        @stage(1)
        def _():
            it = i - 1
            v1_all(it).wait_recv()
            for h in range(2):
                project(it, 1 - h)
                if h == 0:
                    fa(it).start()
                for d in range(2):
                    ra(it, 1 - h, d).start()
            v0(it).wait_send()

        @stage(2)
        def _():
            it = i - 2
            k = it % NS
            fa(it).wait_recv()
            sums = part[k, 1, :, zh, :, rest].astype(F32) + far_in[k].astype(F32)
            far[k] = sums.astype(BF16)
            for d in range(3):
                fb(it, d).start()

        return 0

    lax.fori_loop(1, ITEMS + 8, run, 0)

    total = jnp.sum(squares[...].reshape(128, 128).T, axis=0, keepdims=True)
    sq[...] = jnp.broadcast_to(total, (8, 128))
    sums = []
    for z in range(2):
        for k in range(4):
            for c in range(2):
                if (z, k, c) != (0, 0, 0):
                    dev = at_row((zh + z) % 2, (y + k) % 4, (core + c) % 2)
                    sums.append(send(sq, sq_in.at[row], n_s.at[0], n_r.at[0], dev))
    for c in sums:
        c.start()
    sq_in[row] = sq[...]

    def turn(side, r):
        cols = pl.ds(pl.multiple_of(side * HALF + r * 128, 128), 128)
        return upd[:, :, cols].reshape(128, 128).T

    for r in range(HALF // 128):
        turned[r * 128 : (r + 1) * 128, :] = turn(1 - core, r)
    swap = send(turned, turned_in, u_s.at[0], u_r.at[0], pair)
    swap.start()
    for r in range(HALF // 128):
        out_ref[r * 128 : (r + 1) * 128, pl.ds(pl.multiple_of(core * 128, 128), 128)] = turn(core, r)
    swap.wait_recv()
    out_ref[:, pl.ds(pl.multiple_of((1 - core) * 128, 128), 128)] = turned_in[...]
    others = sq_in.at[pl.ds(0, 15)]
    sums_all = send(others, others, n_s.at[0], n_r.at[0], zl_dev)
    sums_all.wait_recv()
    for c in range(2):
        total = sq_in[c, 0:1, :]
        for r in range(c + 2, 16, 2):
            total = total + sq_in[r, 0:1, :]
        norm_ref[c : c + 1, :] = jnp.sqrt(total)
    for c in (*pairs, swap, sums_all):
        c.wait_send()


def on_device(rotation, gradient):
    dma = pltpu.SemaphoreType.DMA

    def both(shape):
        return [dma(shape), dma(shape)]

    quarters = (4, 2, CH, BLK)
    updated, norms = pl.pallas_call(
        step_kernel,
        name="cayley_step",
        out_shape=(
            jax.ShapeDtypeStruct((HALF, 256), F32),
            jax.ShapeDtypeStruct((2, 128), F32),
        ),
        in_specs=[pl.BlockSpec(memory_space=pl.ANY)] * 2,
        out_specs=(
            pl.BlockSpec(memory_space=pltpu.VMEM),
            pl.BlockSpec(memory_space=pltpu.VMEM),
        ),
        scratch_shapes=[
            pltpu.VMEM((BLK, BLK), BF16),
            pltpu.VMEM((BLK, BLK), BF16),
            pltpu.VMEM((NS, CH, BLK), BF16),
            pltpu.VMEM((NS, CH, HALF), BF16),
            pltpu.VMEM((NS, *quarters), BF16),
            pltpu.VMEM((NS, 2, *quarters), BF16),
            pltpu.VMEM((NS, 2, *quarters), BF16),
            pltpu.VMEM((NS, 2, 2, CH, BLK), BF16),
            pltpu.VMEM((NS, 2, 2, CH, BLK), BF16),
            pltpu.VMEM((NS, 2, 2, 2, CH, BLK), BF16),
            pltpu.VMEM((NS, 2, 2, CH, BLK), BF16),
            pltpu.VMEM((NS, 4, CH, BLK - CUT), BF16),
            pltpu.VMEM((NS, 4, CH, BLK - CUT), BF16),
            pltpu.VMEM((NS, 3, CH, BLK - CUT), BF16),
            pltpu.VMEM((NS, *quarters), BF16),
            pltpu.VMEM((NS, 3, 2, CH, BLK), BF16),
            pltpu.VMEM((NS, CH, BLK), F32),
            pltpu.VMEM((NS, CH, BLK), BF16),
            pltpu.VMEM((NS, CH, BLK), BF16),
            pltpu.VMEM((NS, CH, BLK), F32),
            pltpu.VMEM((NS, CH, 128), F32),
            pltpu.VMEM((HALF, 128), F32),
            pltpu.VMEM((HALF, 128), F32),
            pltpu.VMEM((8, 128), F32),
            pltpu.VMEM((16, 8, 128), F32),
            dma((2,)),
            *both((3,)),
            *both((NS,)),
            *both((NS,)),
            *both((NQ, 2)),
            *both((NQ, 2)),
            *both((NQ, 2)),
            *both((NL, 2)),
            *both((NL, 2)),
            *both((NL,)),
            *both((NQ,)),
            *both((NQ,)),
            *both((NL,)),
            *both((NL,)),
            *both((NL,)),
            *both((1,)),
            *both((1,)),
        ],
        compiler_params=pltpu.CompilerParams(
            collective_id=1, has_side_effects=True, vmem_limit_bytes=53 * 1024 * 1024
        ),
        cost_estimate=pl.CostEstimate(
            flops=20_000_000_000, bytes_accessed=3_000_000, transcendentals=0
        ),
    )(rotation, gradient)
    return updated, norms.reshape(256)


def solution(mesh):
    placed = (P("row", "col"), P("row", "col"))
    return jax.shard_map(
        on_device,
        mesh=mesh,
        in_specs=placed,
        out_specs=(P("row", "col"), P("col")),
        check_vma=False,
    )
```

```python
import jax
import jax.numpy as jnp
from jax import lax
from jax.experimental import pallas as pl
from jax.experimental.pallas import tpu as pltpu
from jax.sharding import PartitionSpec as P

MESH = pl.DeviceIdType.MESH
F32 = jnp.float32
BF16 = jnp.bfloat16
NS = 8
CH = 16
BLK = 1024
HALF = 512
TILE = 1024
ITEMS = 2 * NS
NQ = 2
NL = 4
CUT = 256
WIDE = (BLK, CUT)
LATE = ITEMS - 1


def step_kernel(
    rot_hbm, grad_hbm, out_ref, norm_ref,
    rot, grad, base, base_out, panel, part, full, mine, ring_a, ring_b, swapped, far, far_in, far_y,
    term, term_in, kept, tail, tail_in, upd, squares, turned, turned_in, sq, sq_in,
    load_sem, pair_s, pair_r, v0_s, v0_r, v1_s, v1_r, a_s, a_r, b_s, b_r, z_s, z_r,
    c_s, c_r, e_s, e_r, fa_s, fa_r, fb_s, fb_r, fc_s, fc_r, fd_s, fd_r, t_s, t_r, w_s, w_r, u_s, u_r, n_s, n_r,
):
    row = lax.axis_index("row")
    col = lax.axis_index("col")
    core, y, zh = row % 2, (row // 2) % 4, row // 8
    x, zl = col // 2, col % 2
    up, across, down = (y + 1) % 4, (y + 2) % 4, (y + 3) % 4

    def at_row(zh_, y_, core_):
        return {"row": zh_ * 8 + y_ * 2 + core_, "col": col}

    def at_col(x_, zl_):
        return {"row": row, "col": x_ * 2 + zl_}

    pair = at_row(zh, y, 1 - core)
    y_dev = (at_row(zh, up, core), at_row(zh, down, core))
    y_q = (up, down)
    y_all = tuple(at_row(zh, (y + k) % 4, core) for k in (1, 2, 3))
    z_dev = at_row(1 - zh, y, core)
    x_all = tuple(at_col((x + k) % 4, zl) for k in (1, 2, 3))
    x_far = tuple(at_col((x + k) % 4, 1 - zl) for k in (1, 2, 3))
    zl_dev = at_col(x, 1 - zl)
    zl_pair = {"row": zh * 8 + y * 2 + 1 - core, "col": x * 2 + 1 - zl}

    def send(src, dst, s, r, dev):
        return pltpu.make_async_remote_copy(
            src_ref=src, dst_ref=dst, send_sem=s, recv_sem=r, device_id=dev, device_id_type=MESH
        )

    own_rows = pl.ds(pl.multiple_of(core * HALF, HALF), HALF)
    other_rows = pl.ds(pl.multiple_of((1 - core) * HALF, HALF), HALF)
    loads = [
        pltpu.make_async_copy(rot_hbm, rot.at[own_rows], load_sem.at[0]),
        pltpu.make_async_copy(grad_hbm, grad.at[own_rows], load_sem.at[1]),
    ]
    for c in loads:
        c.start()

    barrier = pltpu.get_barrier_semaphore()
    peers = (pair, *y_dev, z_dev, *x_all, zl_dev, zl_pair)
    for dev in peers:
        pl.semaphore_signal(barrier, inc=1, device_id=dev, device_id_type=MESH)

    pick = lax.broadcasted_iota(jnp.int32, (128, HALF), 1) == 4 * lax.broadcasted_iota(
        jnp.int32, (128, HALF), 0
    )
    pick = pick.astype(F32).astype(BF16)

    def picked(side):
        cols = pl.ds(pl.multiple_of(side * HALF, HALF), HALF)
        return (
            lax.dot_general(
                pick, rot[own_rows, cols], (((1,), (1,)), ((), ())), preferred_element_type=F32
            )
            .astype(BF16)
            .reshape(NS, CH, HALF)
        )

    loads[0].wait()
    base_out[...] = picked(1 - core)
    base[:, :, own_rows] = picked(core)
    panel[0, x, zl, :, own_rows] = base[0, :, own_rows]
    loads[1].wait()

    pl.semaphore_wait(barrier, len(peers))
    pairs = [
        send(base_out, base.at[:, :, own_rows], pair_s.at[0], pair_r.at[0], pair),
        send(rot.at[own_rows], rot.at[own_rows], pair_s.at[1], pair_r.at[1], pair),
        send(grad.at[own_rows], grad.at[own_rows], pair_s.at[2], pair_r.at[2], pair),
    ]
    pairs[0].start()
    there = panel.at[0, x, zl, :, own_rows]
    send(there, there, v0_s.at[0], v0_r.at[0], zl_dev).start()
    send(base_out.at[0], there, v0_s.at[0], v0_r.at[0], zl_pair).start()
    for c in pairs[1:]:
        c.start()
    pairs[0].wait_recv()

    def first(h):
        return pl.ds(0, WIDE[h])

    rest = pl.ds(CUT, BLK - CUT)

    def v0(i):
        k = i % NS
        return send(panel.at[k, x, zl], panel.at[k, x, zl], v0_s.at[k], v0_r.at[k], zl_dev)

    def v1(i, d):
        k = i % NS
        return send(panel.at[k, x], panel.at[k, x], v1_s.at[k], v1_r.at[k], x_all[d])

    def v1_all(i):
        k = i % NS
        return send(term_in.at[k], term_in.at[k], v1_s.at[k], v1_r.at[k], zl_dev)

    def ra(i, h, d):
        k, q = i % NS, i % NL
        return send(
            part.at[k, h, across, d, :, first(h)],
            ring_a.at[k, h, d, :, first(h)],
            a_s.at[q, h],
            a_r.at[q, h],
            y_dev[d],
        )

    def ra_all(i, h):
        k, q = i % NS, i % NL
        ref = ring_a.at[k, h, :, :, first(h)]
        return send(ref, ref, a_s.at[q, h], a_r.at[q, h], zl_dev)

    def rb(i, h, d):
        k, q = i % NS, i % NQ
        return send(
            part.at[k, h, y_q[d], :, :, first(h)],
            ring_b.at[k, h, d, :, :, first(h)],
            b_s.at[q, h],
            b_r.at[q, h],
            y_dev[d],
        )

    def rb_all(i, h):
        k, q = i % NS, i % NQ
        ref = ring_b.at[k, h, :, :, :, first(h)]
        return send(ref, ref, b_s.at[q, h], b_r.at[q, h], zl_dev)

    def zx(i, h):
        k, q = i % NS, i % NQ
        return send(
            mine.at[k, h, :, :, first(h)],
            swapped.at[k, h, :, :, first(h)],
            z_s.at[q, h],
            z_r.at[q, h],
            z_dev,
        )

    def ga(i, h, d):
        k, q = i % NS, i % NL
        place = full.at[k, h, y, :, :, first(h)]
        return send(place, place, c_s.at[q, h], c_r.at[q, h], y_dev[d])

    def ga_all(i, h):
        k, q = i % NS, i % NL
        ref = ring_b.at[k, h, :, :, :, first(h)]
        return send(ref, ref, c_s.at[q, h], c_r.at[q, h], zl_dev)

    def gb(i, h, d):
        k, q = i % NS, i % NL
        place = full.at[k, h, y_q[1 - d], d, :, first(h)]
        return send(place, place, e_s.at[q, h], e_r.at[q, h], y_dev[d])

    def gb_all(i, h):
        k, q = i % NS, i % NL
        ref = ring_a.at[k, h, :, :, first(h)]
        return send(ref, ref, e_s.at[q, h], e_r.at[q, h], zl_dev)

    def fa(i):
        k, q = i % NS, i % NL
        return send(
            part.at[k, 1, :, 1 - zh, :, rest], far_in.at[k], fa_s.at[q], fa_r.at[q], z_dev
        )

    def fb(i, d):
        k, q = i % NS, i % NQ
        return send(
            far.at[k, (y + d + 1) % 4], far_y.at[k, d], fb_s.at[q], fb_r.at[q], y_all[d]
        )

    def fb_all(i):
        k, q = i % NS, i % NQ
        return send(far_y.at[k], far_y.at[k], fb_s.at[q], fb_r.at[q], zl_dev)

    def fc(i, d):
        k, q = i % NS, i % NQ
        place = full.at[k, 1, y, zh, :, rest]
        return send(place, place, fc_s.at[q], fc_r.at[q], y_all[d])

    def fc_all(i):
        k, q = i % NS, i % NQ
        return send(far_y.at[k], far_y.at[k], fc_s.at[q], fc_r.at[q], zl_dev)

    def fd(i):
        k, q = i % NS, i % NL
        place = full.at[k, 1, :, zh, :, rest]
        return send(place, place, fd_s.at[q], fd_r.at[q], z_dev)

    def tx(i, d):
        k, q = i % NS, i % NL
        return send(
            term.at[k, (x + d + 1) % 4], term_in.at[k, d], t_s.at[q], t_r.at[q], x_all[d]
        )

    def tx_all(i):
        k, q = i % NS, i % NL
        return send(term_in.at[k], term_in.at[k], t_s.at[q], t_r.at[q], zl_dev)

    def wz(i):
        k, q = i % NS, i % NL
        return send(tail.at[k], tail_in.at[k], w_s.at[q], w_r.at[q], zl_dev)

    panel[0, x, zl, :, other_rows] = base[0, :, other_rows]

    def block_to_all(z):
        place = panel.at[0, x, z]
        for d in range(3):
            send(place, place, v1_s.at[0], v1_r.at[0], x_all[d]).start()

    block_to_all(zl)
    for j in range(1, NS):
        panel[j, x, zl] = base[j]
    for j in range(1, NS):
        v0(j).start()
    v0(0).wait_recv()
    block_to_all(1 - zl)
    for j in range(1, NS):
        v0(j).wait_recv()
        for d in range(3):
            v1(j, d).start()
    pairs[1].wait_recv()
    pairs[2].wait_recv()

    def project(i, h):
        k = i % NS
        held = (rot, grad)[h]
        lhs = panel[k].reshape(8 * CH, BLK)

        @pl.loop(0, BLK // TILE)
        def _(n):
            cols = pl.ds(pl.multiple_of(n * TILE, TILE), TILE)
            z = jnp.dot(lhs, held[:, cols], preferred_element_type=F32)
            part[k, h, :, :, :, cols] = z.astype(BF16).reshape(4, 2, CH, TILE)

    def apply(i):
        k = i % NS

        @pl.loop(0, BLK // TILE)
        def _(n):
            rows = pl.ds(pl.multiple_of(n * TILE, TILE), TILE)
            nt = (((1,), (1,)), ((), ()))
            t = lax.dot_general(
                full[k, 0].reshape(8 * CH, BLK), grad[rows, :], nt, preferred_element_type=F32
            ) - lax.dot_general(
                full[k, 1].reshape(8 * CH, BLK), rot[rows, :], nt, preferred_element_type=F32
            )
            term[k, :, :, :, rows] = t.astype(BF16).reshape(4, 2, CH, TILE)

    def run(i, _):
        def stage(late):
            return pl.when((i >= late) & (i < ITEMS + late))

        @pl.when((i > NS) & (i <= ITEMS))
        def _():
            v0(i - 1).wait_recv()
            for d in range(3):
                v1(i - 1, d).start()

        @stage(5)
        def _():
            it = i - 5
            for h in range(2):
                ga_all(it, h).wait_recv()
                for d in range(2):
                    gb(it, h, d).start()
            for h in range(2):
                zx(it, h).wait_send()
            fc_all(it).wait_send()

        @stage(4)
        def _():
            it = i - 4
            k = it % NS
            for h in range(2):
                zx(it, h).wait_recv()
                w = first(h)
                z = mine[k, h, :, :, w].astype(F32) + swapped[k, h, :, :, w].astype(F32)
                full[k, h, y, :, :, w] = z.astype(BF16)
                for d in range(2):
                    ga(it, h, d).start()
            for h in range(2):
                rb_all(it, h).wait_send()

        @stage(3)
        def _():
            it = i - 3
            k = it % NS
            for h in range(2):
                rb_all(it, h).wait_recv()
                w = first(h)
                s = part[k, h, y, :, :, w].astype(F32) + (
                    ring_b[k, h, 0, :, :, w].astype(F32) + ring_b[k, h, 1, :, :, w].astype(F32)
                )
                mine[k, h, :, :, w] = s.astype(BF16)
                zx(it, h).start()
            for h in range(2):
                ra_all(it, h).wait_send()

        @stage(8)
        def _():
            it = i - 8
            k = it % NS
            wz(it).wait_recv()
            applied = kept[k] + tail_in[k].astype(F32)
            b = base[k].astype(F32)

            @pl.when(i < ITEMS)
            def _():
                first = b + 0.25 * applied
                panel[k, x, zl] = (b + first).astype(BF16)
                v0(i).start()

            @pl.when(i >= ITEMS)
            def _():
                new = b + 0.125 * applied
                upd[k] = new
                lanes = new[:, :128] * new[:, :128]
                for r in range(1, BLK // 128):
                    lane = new[:, r * 128 : (r + 1) * 128]
                    lanes = lanes + lane * lane
                squares[k] = lanes

            tx_all(it).wait_send()
            wz(it).wait_send()

        @stage(2)
        def _():
            it = i - 2
            k = it % NS
            for h in range(2):
                w = first(h)
                ra_all(it, h).wait_recv()
                for d in range(2):
                    there = part[k, h, y_q[d], d, :, w].astype(F32)
                    there = there + ring_a[k, h, d, :, w].astype(F32)
                    part[k, h, y_q[d], d, :, w] = there.astype(BF16)
                    rb(it, h, d).start()
            v1_all(it).wait_send()

        @stage(6)
        def _():
            it = i - 6
            for h in range(2):
                gb_all(it, h).wait_recv()
            fd(it).wait_recv()
            apply(it)
            k, q = it % NS, it % NL

            @pl.when(it < LATE)
            def _():
                for d in range(3):
                    tx(it, d).start()

            @pl.when(it >= LATE)
            def _():
                for d in range(3):
                    for z, dev in ((0, x_all[d]), (1, x_far[d])):
                        src = term.at[k, (x + d + 1) % 4, zl + z - 2 * zl * z]
                        send(src, term_in.at[k, d, z], t_s.at[q], t_r.at[q], dev).start()
                send(term.at[k, x, 1 - zl], tail_in.at[k], w_s.at[q], w_r.at[q], zl_dev).start()

            for h in range(2):
                ga_all(it, h).wait_send()
            fd(it).wait_send()

        @stage(7)
        def _():
            it = i - 7
            k = it % NS
            tx_all(it).wait_recv()

            def summed(z):
                return (term[k, x, z].astype(F32) + term_in[k, 0, z].astype(F32)) + (
                    term_in[k, 1, z].astype(F32) + term_in[k, 2, z].astype(F32)
                )

            @pl.when(it < LATE)
            def _():
                tail[k] = summed(1 - zl).astype(BF16)
                wz(it).start()
                kept[k] = summed(zl)

            @pl.when(it >= LATE)
            def _():
                total = term[k, x, zl].astype(F32)
                for d in range(3):
                    total = total + (term_in[k, d, 0].astype(F32) + term_in[k, d, 1].astype(F32))
                kept[k] = total

            for h in range(2):
                gb_all(it, h).wait_send()

        @stage(4)
        def _():
            it = i - 4
            fc_all(it).wait_recv()
            fd(it).start()
            fb_all(it).wait_send()

        @stage(3)
        def _():
            it = i - 3
            k = it % NS
            fb_all(it).wait_recv()
            s = (far[k, y].astype(F32) + far_y[k, 0].astype(F32)) + (
                far_y[k, 1].astype(F32) + far_y[k, 2].astype(F32)
            )
            full[k, 1, y, zh, :, rest] = s.astype(BF16)
            for d in range(3):
                fc(it, d).start()
            fa(it).wait_send()

        @pl.when((i != NS) & (i <= ITEMS))
        def _():
            it = i - i // (NS + 1)
            v1_all(it).wait_recv()
            for h in range(2):
                project(it, 1 - h)
                if h == 0:
                    fa(it).start()
                for d in range(2):
                    ra(it, 1 - h, d).start()
            v0(it).wait_send()

        @stage(2)
        def _():
            it = i - 2
            k = it % NS
            fa(it).wait_recv()
            sums = part[k, 1, :, zh, :, rest].astype(F32) + far_in[k].astype(F32)
            far[k] = sums.astype(BF16)
            for d in range(3):
                fb(it, d).start()

        return 0

    lax.fori_loop(0, ITEMS + 8, run, 0)

    total = jnp.sum(squares[...].reshape(128, 128).T, axis=0, keepdims=True)
    sq[...] = jnp.broadcast_to(total, (8, 128))
    sums = []
    for z in range(2):
        for k in range(4):
            for c in range(2):
                if (z, k, c) != (0, 0, 0):
                    dev = at_row((zh + z) % 2, (y + k) % 4, (core + c) % 2)
                    sums.append(send(sq, sq_in.at[row], n_s.at[0], n_r.at[0], dev))
    for c in sums:
        c.start()
    sq_in[row] = sq[...]

    def turn(side, r):
        cols = pl.ds(pl.multiple_of(side * HALF + r * 128, 128), 128)
        return upd[:, :, cols].reshape(128, 128).T

    for r in range(HALF // 128):
        turned[r * 128 : (r + 1) * 128, :] = turn(1 - core, r)
    swap = send(turned, turned_in, u_s.at[0], u_r.at[0], pair)
    swap.start()
    for r in range(HALF // 128):
        out_ref[r * 128 : (r + 1) * 128, pl.ds(pl.multiple_of(core * 128, 128), 128)] = turn(core, r)
    swap.wait_recv()
    out_ref[:, pl.ds(pl.multiple_of((1 - core) * 128, 128), 128)] = turned_in[...]
    others = sq_in.at[pl.ds(0, 15)]
    sums_all = send(others, others, n_s.at[0], n_r.at[0], zl_dev)
    sums_all.wait_recv()
    for c in range(2):
        total = sq_in[c, 0:1, :]
        for r in range(c + 2, 16, 2):
            total = total + sq_in[r, 0:1, :]
        norm_ref[c : c + 1, :] = jnp.sqrt(total)
    for c in (*pairs, swap, sums_all):
        c.wait_send()


def on_device(rotation, gradient):
    dma = pltpu.SemaphoreType.DMA

    def both(shape):
        return [dma(shape), dma(shape)]

    quarters = (4, 2, CH, BLK)
    updated, norms = pl.pallas_call(
        step_kernel,
        name="cayley_step",
        out_shape=(
            jax.ShapeDtypeStruct((HALF, 256), F32),
            jax.ShapeDtypeStruct((2, 128), F32),
        ),
        in_specs=[pl.BlockSpec(memory_space=pl.ANY)] * 2,
        out_specs=(
            pl.BlockSpec(memory_space=pltpu.VMEM),
            pl.BlockSpec(memory_space=pltpu.VMEM),
        ),
        scratch_shapes=[
            pltpu.VMEM((BLK, BLK), BF16),
            pltpu.VMEM((BLK, BLK), BF16),
            pltpu.VMEM((NS, CH, BLK), BF16),
            pltpu.VMEM((NS, CH, HALF), BF16),
            pltpu.VMEM((NS, *quarters), BF16),
            pltpu.VMEM((NS, 2, *quarters), BF16),
            pltpu.VMEM((NS, 2, *quarters), BF16),
            pltpu.VMEM((NS, 2, 2, CH, BLK), BF16),
            pltpu.VMEM((NS, 2, 2, CH, BLK), BF16),
            pltpu.VMEM((NS, 2, 2, 2, CH, BLK), BF16),
            pltpu.VMEM((NS, 2, 2, CH, BLK), BF16),
            pltpu.VMEM((NS, 4, CH, BLK - CUT), BF16),
            pltpu.VMEM((NS, 4, CH, BLK - CUT), BF16),
            pltpu.VMEM((NS, 3, CH, BLK - CUT), BF16),
            pltpu.VMEM((NS, *quarters), BF16),
            pltpu.VMEM((NS, 3, 2, CH, BLK), BF16),
            pltpu.VMEM((NS, CH, BLK), F32),
            pltpu.VMEM((NS, CH, BLK), BF16),
            pltpu.VMEM((NS, CH, BLK), BF16),
            pltpu.VMEM((NS, CH, BLK), F32),
            pltpu.VMEM((NS, CH, 128), F32),
            pltpu.VMEM((HALF, 128), F32),
            pltpu.VMEM((HALF, 128), F32),
            pltpu.VMEM((8, 128), F32),
            pltpu.VMEM((16, 8, 128), F32),
            dma((2,)),
            *both((3,)),
            *both((NS,)),
            *both((NS,)),
            *both((NL, 2)),
            *both((NQ, 2)),
            *both((NQ, 2)),
            *both((NL, 2)),
            *both((NL, 2)),
            *both((NL,)),
            *both((NQ,)),
            *both((NQ,)),
            *both((NL,)),
            *both((NL,)),
            *both((NL,)),
            *both((1,)),
            *both((1,)),
        ],
        compiler_params=pltpu.CompilerParams(
            collective_id=1, has_side_effects=True, vmem_limit_bytes=53 * 1024 * 1024
        ),
        cost_estimate=pl.CostEstimate(
            flops=20_000_000_000, bytes_accessed=3_000_000, transcendentals=0
        ),
    )(rotation, gradient)
    return updated, norms.reshape(256)


def solution(mesh):
    placed = (P("row", "col"), P("row", "col"))
    return jax.shard_map(
        on_device,
        mesh=mesh,
        in_specs=placed,
        out_specs=(P("row", "col"), P("col")),
        check_vma=False,
    )
```

```python
import jax
import jax.numpy as jnp
from jax import lax
from jax.experimental import pallas as pl
from jax.experimental.pallas import tpu as pltpu
from jax.sharding import PartitionSpec as P

MESH = pl.DeviceIdType.MESH
F32 = jnp.float32
BF16 = jnp.bfloat16
NS = 8
CH = 16
BLK = 1024
HALF = 512
TILE = 1024
ITEMS = 2 * NS
NQ = 2
NL = 4
CUT = 256
WIDE = (BLK, CUT)
LATE = ITEMS - 1


def step_kernel(
    rot_hbm, grad_hbm, out_ref, norm_ref,
    rot, grad, base, base_out, panel, part, full, mine, ring_a, ring_b, swapped, far, far_in, far_y,
    term, term_in, kept, tail, tail_in, upd, squares, turned, turned_in, sq, sq_in,
    load_sem, pair_s, pair_r, v0_s, v0_r, v1_s, v1_r, a_s, a_r, b_s, b_r, z_s, z_r,
    c_s, c_r, e_s, e_r, fa_s, fa_r, fb_s, fb_r, fc_s, fc_r, fd_s, fd_r, t_s, t_r, w_s, w_r, u_s, u_r, n_s, n_r,
):
    row = lax.axis_index("row")
    col = lax.axis_index("col")
    core, y, zh = row % 2, (row // 2) % 4, row // 8
    x, zl = col // 2, col % 2
    up, across, down = (y + 1) % 4, (y + 2) % 4, (y + 3) % 4

    def at_row(zh_, y_, core_):
        return {"row": zh_ * 8 + y_ * 2 + core_, "col": col}

    def at_col(x_, zl_):
        return {"row": row, "col": x_ * 2 + zl_}

    pair = at_row(zh, y, 1 - core)
    y_dev = (at_row(zh, up, core), at_row(zh, down, core))
    y_q = (up, down)
    y_all = tuple(at_row(zh, (y + k) % 4, core) for k in (1, 2, 3))
    z_dev = at_row(1 - zh, y, core)
    x_all = tuple(at_col((x + k) % 4, zl) for k in (1, 2, 3))
    x_far = tuple(at_col((x + k) % 4, 1 - zl) for k in (1, 2, 3))
    zl_dev = at_col(x, 1 - zl)
    zl_pair = {"row": zh * 8 + y * 2 + 1 - core, "col": x * 2 + 1 - zl}

    def send(src, dst, s, r, dev):
        return pltpu.make_async_remote_copy(
            src_ref=src, dst_ref=dst, send_sem=s, recv_sem=r, device_id=dev, device_id_type=MESH
        )

    own_rows = pl.ds(pl.multiple_of(core * HALF, HALF), HALF)
    other_rows = pl.ds(pl.multiple_of((1 - core) * HALF, HALF), HALF)
    loads = [
        pltpu.make_async_copy(rot_hbm, rot.at[own_rows], load_sem.at[0]),
        pltpu.make_async_copy(grad_hbm, grad.at[own_rows], load_sem.at[1]),
    ]
    for c in loads:
        c.start()

    barrier = pltpu.get_barrier_semaphore()
    peers = (pair, *y_dev, z_dev, *x_all, zl_dev, zl_pair)
    for dev in peers:
        pl.semaphore_signal(barrier, inc=1, device_id=dev, device_id_type=MESH)

    pick = lax.broadcasted_iota(jnp.int32, (128, HALF), 1) == 4 * lax.broadcasted_iota(
        jnp.int32, (128, HALF), 0
    )
    pick = pick.astype(F32).astype(BF16)

    def picked(side):
        cols = pl.ds(pl.multiple_of(side * HALF, HALF), HALF)
        return (
            lax.dot_general(
                pick, rot[own_rows, cols], (((1,), (1,)), ((), ())), preferred_element_type=F32
            )
            .astype(BF16)
            .reshape(NS, CH, HALF)
        )

    loads[0].wait()
    base_out[...] = picked(1 - core)
    base[:, :, own_rows] = picked(core)
    panel[0, x, zl, :, own_rows] = base[0, :, own_rows]
    loads[1].wait()

    pl.semaphore_wait(barrier, len(peers))
    pairs = [
        send(base_out, base.at[:, :, own_rows], pair_s.at[0], pair_r.at[0], pair),
        send(rot.at[own_rows], rot.at[own_rows], pair_s.at[1], pair_r.at[1], pair),
        send(grad.at[own_rows], grad.at[own_rows], pair_s.at[2], pair_r.at[2], pair),
    ]
    pairs[0].start()
    there = panel.at[0, x, zl, :, own_rows]
    send(there, there, v0_s.at[0], v0_r.at[0], zl_dev).start()
    send(base_out.at[0], there, v0_s.at[0], v0_r.at[0], zl_pair).start()
    for c in pairs[1:]:
        c.start()
    pairs[0].wait_recv()

    def first(h):
        return pl.ds(0, WIDE[h])

    rest = pl.ds(CUT, BLK - CUT)

    def v0(i):
        k = i % NS
        return send(panel.at[k, x, zl], panel.at[k, x, zl], v0_s.at[k], v0_r.at[k], zl_dev)

    def v1(i, d):
        k = i % NS
        return send(panel.at[k, x], panel.at[k, x], v1_s.at[k], v1_r.at[k], x_all[d])

    def v1_all(i):
        k = i % NS
        return send(term_in.at[k], term_in.at[k], v1_s.at[k], v1_r.at[k], zl_dev)

    def ra(i, h, d):
        k, q = i % NS, i % NL
        return send(
            part.at[k, h, across, d, :, first(h)],
            ring_a.at[k, h, d, :, first(h)],
            a_s.at[q, h],
            a_r.at[q, h],
            y_dev[d],
        )

    def ra_all(i, h):
        k, q = i % NS, i % NL
        ref = ring_a.at[k, h, :, :, first(h)]
        return send(ref, ref, a_s.at[q, h], a_r.at[q, h], zl_dev)

    def rb(i, h, d):
        k, q = i % NS, i % NQ
        return send(
            part.at[k, h, y_q[d], :, :, first(h)],
            ring_b.at[k, h, d, :, :, first(h)],
            b_s.at[q, h],
            b_r.at[q, h],
            y_dev[d],
        )

    def rb_all(i, h):
        k, q = i % NS, i % NQ
        ref = ring_b.at[k, h, :, :, :, first(h)]
        return send(ref, ref, b_s.at[q, h], b_r.at[q, h], zl_dev)

    def zx(i, h):
        k, q = i % NS, i % NQ
        return send(
            mine.at[k, h, :, :, first(h)],
            swapped.at[k, h, :, :, first(h)],
            z_s.at[q, h],
            z_r.at[q, h],
            z_dev,
        )

    def ga(i, h, d):
        k, q = i % NS, i % NL
        place = full.at[k, h, y, :, :, first(h)]
        return send(place, place, c_s.at[q, h], c_r.at[q, h], y_dev[d])

    def ga_all(i, h):
        k, q = i % NS, i % NL
        ref = ring_b.at[k, h, :, :, :, first(h)]
        return send(ref, ref, c_s.at[q, h], c_r.at[q, h], zl_dev)

    def gb(i, h, d):
        k, q = i % NS, i % NL
        place = full.at[k, h, y_q[1 - d], d, :, first(h)]
        return send(place, place, e_s.at[q, h], e_r.at[q, h], y_dev[d])

    def gb_all(i, h):
        k, q = i % NS, i % NL
        ref = ring_a.at[k, h, :, :, first(h)]
        return send(ref, ref, e_s.at[q, h], e_r.at[q, h], zl_dev)

    def fa(i):
        k, q = i % NS, i % NL
        return send(
            part.at[k, 1, :, 1 - zh, :, rest], far_in.at[k], fa_s.at[q], fa_r.at[q], z_dev
        )

    def fb(i, d):
        k, q = i % NS, i % NQ
        return send(
            far.at[k, (y + d + 1) % 4], far_y.at[k, d], fb_s.at[q], fb_r.at[q], y_all[d]
        )

    def fb_all(i):
        k, q = i % NS, i % NQ
        return send(far_y.at[k], far_y.at[k], fb_s.at[q], fb_r.at[q], zl_dev)

    def fc(i, d):
        k, q = i % NS, i % NQ
        place = full.at[k, 1, y, zh, :, rest]
        return send(place, place, fc_s.at[q], fc_r.at[q], y_all[d])

    def fc_all(i):
        k, q = i % NS, i % NQ
        return send(far_y.at[k], far_y.at[k], fc_s.at[q], fc_r.at[q], zl_dev)

    def fd(i):
        k, q = i % NS, i % NL
        place = full.at[k, 1, :, zh, :, rest]
        return send(place, place, fd_s.at[q], fd_r.at[q], z_dev)

    def tx(i, d):
        k, q = i % NS, i % NL
        return send(
            term.at[k, (x + d + 1) % 4], term_in.at[k, d], t_s.at[q], t_r.at[q], x_all[d]
        )

    def tx_all(i):
        k, q = i % NS, i % NL
        return send(term_in.at[k], term_in.at[k], t_s.at[q], t_r.at[q], zl_dev)

    def wz(i):
        k, q = i % NS, i % NL
        return send(tail.at[k], tail_in.at[k], w_s.at[q], w_r.at[q], zl_dev)

    panel[0, x, zl, :, other_rows] = base[0, :, other_rows]

    def block_to_all(z):
        place = panel.at[0, x, z]
        for d in range(3):
            send(place, place, v1_s.at[0], v1_r.at[0], x_all[d]).start()

    block_to_all(zl)
    for j in range(1, NS):
        panel[j, x, zl] = base[j]
    for j in range(1, NS):
        v0(j).start()
    v0(0).wait_recv()
    block_to_all(1 - zl)
    for j in range(1, NS):
        v0(j).wait_recv()
        for d in range(3):
            v1(j, d).start()
    pairs[1].wait_recv()
    pairs[2].wait_recv()

    def project(i, h):
        k = i % NS
        held = (rot, grad)[h]
        lhs = panel[k].reshape(8 * CH, BLK)

        @pl.loop(0, BLK // TILE)
        def _(n):
            cols = pl.ds(pl.multiple_of(n * TILE, TILE), TILE)
            z = jnp.dot(lhs, held[:, cols], preferred_element_type=F32)
            part[k, h, :, :, :, cols] = z.astype(BF16).reshape(4, 2, CH, TILE)

    def apply(i):
        k = i % NS

        @pl.loop(0, BLK // TILE)
        def _(n):
            rows = pl.ds(pl.multiple_of(n * TILE, TILE), TILE)
            nt = (((1,), (1,)), ((), ()))
            t = lax.dot_general(
                full[k, 0].reshape(8 * CH, BLK), grad[rows, :], nt, preferred_element_type=F32
            ) - lax.dot_general(
                full[k, 1].reshape(8 * CH, BLK), rot[rows, :], nt, preferred_element_type=F32
            )
            term[k, :, :, :, rows] = t.astype(BF16).reshape(4, 2, CH, TILE)

    def run(i, _):
        def stage(late):
            return pl.when((i >= late) & (i < ITEMS + late))

        @pl.when((i > NS) & (i <= ITEMS))
        def _():
            v0(i - 1).wait_recv()
            for d in range(3):
                v1(i - 1, d).start()

        @stage(5)
        def _():
            it = i - 5
            for h in range(2):
                ga_all(it, h).wait_recv()
                for d in range(2):
                    gb(it, h, d).start()
            for h in range(2):
                zx(it, h).wait_send()
            fc_all(it).wait_send()

        @stage(4)
        def _():
            it = i - 4
            k = it % NS
            for h in range(2):
                zx(it, h).wait_recv()
                w = first(h)
                z = mine[k, h, :, :, w].astype(F32) + swapped[k, h, :, :, w].astype(F32)
                full[k, h, y, :, :, w] = z.astype(BF16)
                for d in range(2):
                    ga(it, h, d).start()
            for h in range(2):
                rb_all(it, h).wait_send()

        @stage(3)
        def _():
            it = i - 3
            k = it % NS
            for h in range(2):
                rb_all(it, h).wait_recv()
                w = first(h)
                s = part[k, h, y, :, :, w].astype(F32) + (
                    ring_b[k, h, 0, :, :, w].astype(F32) + ring_b[k, h, 1, :, :, w].astype(F32)
                )
                mine[k, h, :, :, w] = s.astype(BF16)
                zx(it, h).start()
            for h in range(2):
                ra_all(it, h).wait_send()

        @stage(8)
        def _():
            it = i - 8
            k = it % NS
            wz(it).wait_recv()
            applied = kept[k] + tail_in[k].astype(F32)
            b = base[k].astype(F32)

            @pl.when(i < ITEMS)
            def _():
                first = b + 0.25 * applied
                panel[k, x, zl] = (b + first).astype(BF16)
                v0(i).start()

            @pl.when(i >= ITEMS)
            def _():
                new = b + 0.125 * applied
                upd[k] = new
                lanes = new[:, :128] * new[:, :128]
                for r in range(1, BLK // 128):
                    lane = new[:, r * 128 : (r + 1) * 128]
                    lanes = lanes + lane * lane
                squares[k] = lanes

            tx_all(it).wait_send()
            wz(it).wait_send()

        @stage(2)
        def _():
            it = i - 2
            k = it % NS
            for h in range(2):
                w = first(h)
                ra_all(it, h).wait_recv()
                for d in range(2):
                    there = part[k, h, y_q[d], d, :, w].astype(F32)
                    there = there + ring_a[k, h, d, :, w].astype(F32)
                    part[k, h, y_q[d], d, :, w] = there.astype(BF16)
                    rb(it, h, d).start()
            v1_all(it).wait_send()

        @stage(6)
        def _():
            it = i - 6
            for h in range(2):
                gb_all(it, h).wait_recv()
            fd(it).wait_recv()
            apply(it)
            k, q = it % NS, it % NL

            @pl.when(it < LATE)
            def _():
                for d in range(3):
                    tx(it, d).start()

            @pl.when(it >= LATE)
            def _():
                for d in range(3):
                    for z, dev in ((0, x_all[d]), (1, x_far[d])):
                        src = term.at[k, (x + d + 1) % 4, zl + z - 2 * zl * z]
                        send(src, term_in.at[k, d, z], t_s.at[q], t_r.at[q], dev).start()
                send(term.at[k, x, 1 - zl], tail_in.at[k], w_s.at[q], w_r.at[q], zl_dev).start()

            for h in range(2):
                ga_all(it, h).wait_send()
            fd(it).wait_send()

        @stage(7)
        def _():
            it = i - 7
            k = it % NS
            tx_all(it).wait_recv()

            def summed(z):
                return (term[k, x, z].astype(F32) + term_in[k, 0, z].astype(F32)) + (
                    term_in[k, 1, z].astype(F32) + term_in[k, 2, z].astype(F32)
                )

            @pl.when(it < LATE)
            def _():
                tail[k] = summed(1 - zl).astype(BF16)
                wz(it).start()
                kept[k] = summed(zl)

            @pl.when(it >= LATE)
            def _():
                total = term[k, x, zl].astype(F32)
                for d in range(3):
                    total = total + (term_in[k, d, 0].astype(F32) + term_in[k, d, 1].astype(F32))
                kept[k] = total

            for h in range(2):
                gb_all(it, h).wait_send()

        @stage(4)
        def _():
            it = i - 4
            fc_all(it).wait_recv()
            fd(it).start()
            fb_all(it).wait_send()

        @stage(3)
        def _():
            it = i - 3
            k = it % NS
            fb_all(it).wait_recv()
            s = (far[k, y].astype(F32) + far_y[k, 0].astype(F32)) + (
                far_y[k, 1].astype(F32) + far_y[k, 2].astype(F32)
            )
            full[k, 1, y, zh, :, rest] = s.astype(BF16)
            for d in range(3):
                fc(it, d).start()
            fa(it).wait_send()

        @pl.when((i != NS) & (i <= ITEMS))
        def _():
            it = i - i // (NS + 1)
            v1_all(it).wait_recv()
            for h in range(2):
                project(it, 1 - h)
                if h == 0:
                    fa(it).start()
                for d in range(2):
                    ra(it, 1 - h, d).start()
            v0(it).wait_send()

        @stage(2)
        def _():
            it = i - 2
            k = it % NS
            fa(it).wait_recv()
            sums = part[k, 1, :, zh, :, rest].astype(F32) + far_in[k].astype(F32)
            far[k] = sums.astype(BF16)
            for d in range(3):
                fb(it, d).start()

        return 0

    lax.fori_loop(0, ITEMS + 8, run, 0)

    total = jnp.sum(squares[...].reshape(128, 128).T, axis=0, keepdims=True)
    sq[...] = jnp.broadcast_to(total, (8, 128))
    sums = []
    for z in (1, 0):
        for k in (2, 1, 3, 0):
            for c in (1, 0):
                if (z, k, c) != (0, 0, 0):
                    dev = at_row((zh + z) % 2, (y + k) % 4, (core + c) % 2)
                    sums.append(send(sq, sq_in.at[row], n_s.at[0], n_r.at[0], dev))
    for c in sums:
        c.start()
    sq_in[row] = sq[...]

    def turn(side, r):
        cols = pl.ds(pl.multiple_of(side * HALF + r * 128, 128), 128)
        return upd[:, :, cols].reshape(128, 128).T

    for r in range(HALF // 128):
        turned[r * 128 : (r + 1) * 128, :] = turn(1 - core, r)
    swap = send(turned, turned_in, u_s.at[0], u_r.at[0], pair)
    swap.start()
    for r in range(HALF // 128):
        out_ref[r * 128 : (r + 1) * 128, pl.ds(pl.multiple_of(core * 128, 128), 128)] = turn(core, r)
    swap.wait_recv()
    out_ref[:, pl.ds(pl.multiple_of((1 - core) * 128, 128), 128)] = turned_in[...]
    others = sq_in.at[pl.ds(0, 15)]
    sums_all = send(others, others, n_s.at[0], n_r.at[0], zl_dev)
    sums_all.wait_recv()
    for c in range(2):
        total = sq_in[c, 0:1, :]
        for r in range(c + 2, 16, 2):
            total = total + sq_in[r, 0:1, :]
        norm_ref[c : c + 1, :] = jnp.sqrt(total)
    for c in (*pairs, swap, sums_all):
        c.wait_send()


def on_device(rotation, gradient):
    dma = pltpu.SemaphoreType.DMA

    def both(shape):
        return [dma(shape), dma(shape)]

    quarters = (4, 2, CH, BLK)
    updated, norms = pl.pallas_call(
        step_kernel,
        name="cayley_step",
        out_shape=(
            jax.ShapeDtypeStruct((HALF, 256), F32),
            jax.ShapeDtypeStruct((2, 128), F32),
        ),
        in_specs=[pl.BlockSpec(memory_space=pl.ANY)] * 2,
        out_specs=(
            pl.BlockSpec(memory_space=pltpu.VMEM),
            pl.BlockSpec(memory_space=pltpu.VMEM),
        ),
        scratch_shapes=[
            pltpu.VMEM((BLK, BLK), BF16),
            pltpu.VMEM((BLK, BLK), BF16),
            pltpu.VMEM((NS, CH, BLK), BF16),
            pltpu.VMEM((NS, CH, HALF), BF16),
            pltpu.VMEM((NS, *quarters), BF16),
            pltpu.VMEM((NS, 2, *quarters), BF16),
            pltpu.VMEM((NS, 2, *quarters), BF16),
            pltpu.VMEM((NS, 2, 2, CH, BLK), BF16),
            pltpu.VMEM((NS, 2, 2, CH, BLK), BF16),
            pltpu.VMEM((NS, 2, 2, 2, CH, BLK), BF16),
            pltpu.VMEM((NS, 2, 2, CH, BLK), BF16),
            pltpu.VMEM((NS, 4, CH, BLK - CUT), BF16),
            pltpu.VMEM((NS, 4, CH, BLK - CUT), BF16),
            pltpu.VMEM((NS, 3, CH, BLK - CUT), BF16),
            pltpu.VMEM((NS, *quarters), BF16),
            pltpu.VMEM((NS, 3, 2, CH, BLK), BF16),
            pltpu.VMEM((NS, CH, BLK), F32),
            pltpu.VMEM((NS, CH, BLK), BF16),
            pltpu.VMEM((NS, CH, BLK), BF16),
            pltpu.VMEM((NS, CH, BLK), F32),
            pltpu.VMEM((NS, CH, 128), F32),
            pltpu.VMEM((HALF, 128), F32),
            pltpu.VMEM((HALF, 128), F32),
            pltpu.VMEM((8, 128), F32),
            pltpu.VMEM((16, 8, 128), F32),
            dma((2,)),
            *both((3,)),
            *both((NS,)),
            *both((NS,)),
            *both((NL, 2)),
            *both((NQ, 2)),
            *both((NQ, 2)),
            *both((NL, 2)),
            *both((NL, 2)),
            *both((NL,)),
            *both((NQ,)),
            *both((NQ,)),
            *both((NL,)),
            *both((NL,)),
            *both((NL,)),
            *both((1,)),
            *both((1,)),
        ],
        compiler_params=pltpu.CompilerParams(
            collective_id=1, has_side_effects=True, vmem_limit_bytes=53 * 1024 * 1024
        ),
        cost_estimate=pl.CostEstimate(
            flops=20_000_000_000, bytes_accessed=3_000_000, transcendentals=0
        ),
    )(rotation, gradient)
    return updated, norms.reshape(256)


def solution(mesh):
    placed = (P("row", "col"), P("row", "col"))
    return jax.shard_map(
        on_device,
        mesh=mesh,
        in_specs=placed,
        out_specs=(P("row", "col"), P("col")),
        check_vma=False,
    )
```
